32 devices in a mesh: tm: 8 (over y, x, core), space: 4 (over z).
Axes of the slice: x: 2, y: 2, z: 4, core: 2. Of those that a mesh axis runs over, the one named last changes fastest.
Arguments:
- rhs: float32 [16, 1024, 1024], P('tm', 'space'), may hold values from -6 to 6
- guess: float32 [16, 1024, 1024], P('tm', 'space'), may hold values from -6 to 6
- diffusion: float32 [1024, 1024], P('space'), may hold values from 0.2 to 2
Outputs:
- solution: float32 [16, 1024, 1024], P('tm', 'space')
- norms: float32 [6], replicated
The draws below stay inside these ranges and needn't reach their ends.
All inputs are finite; a program needn't handle non-finite values.
Results may differ from the reference program's by a relative error of at most 0.0001.
Values sent between devices are 32-bit elements; how exact they have to be, the bound alone decides.
A program may use at most 64 MiB of HBM per device.

```python
import math
import jax
import jax.numpy as jnp

NY = 1024
LEVELS = 5
NT = 16
NX = 1024


def levels(own_key, extent, split, smallest, high):
    loudness = 1.0
    for dim, shards_of in split:
        steps = jax.random.uniform(jax.random.fold_in(jax.random.fold_in(own_key, 6), dim), (shards_of,), jnp.float32, smallest / len(split), high / len(split))
        loudness = loudness * jnp.repeat(jnp.exp(steps), extent[dim] // shards_of).reshape((-1,) + (1,) * (len(extent) - 1 - dim))
    return loudness


def centred(rng, dims, spread, limit, pieces=(), held_as=jnp.bfloat16):
    gain = levels(rng, dims, pieces, -0.22, 0.18) if pieces else 1.0
    values = jax.random.normal(rng, dims, jnp.float32) * spread * gain
    return jnp.minimum(jnp.maximum(values, -limit), limit).astype(held_as)


def setup_inputs(seed: int = 0) -> dict:
    streams_of = jax.random.split(jax.random.key(seed), 4)
    rhs = centred(streams_of[0], (NT, NX, NY), 1.0, 6.0, ((0, 8), (1, 4)), jnp.float32)
    guess = centred(streams_of[1], (NT, NX, NY), 1.0, 6.0, ((0, 8), (1, 4)), jnp.float32)
    diffusion = jnp.clip(jnp.exp(math.log(2.0) - 2.3025851 * jax.random.uniform(streams_of[2], (NX, NY), jnp.float32) ** levels(streams_of[2], (NX, NY), ((0, 4),), -0.2, 0.2)), 0.2, 2.0)
    return dict(rhs=rhs, guess=guess, diffusion=diffusion)


def neighbours(field):
    padded = jnp.pad(field, ((0, 0), (1, 1), (1, 1)))
    total = padded[:, 2:, 1:-1] + padded[:, :-2, 1:-1]
    total = total + padded[:, 1:-1, 2:] + padded[:, 1:-1, :-2]
    return total

def residual(field, source, scaled, diag):
    before = jnp.concatenate([jnp.zeros_like(field[:1]), field[:-1]], axis=0)
    image = diag * field - scaled * neighbours(field) - before
    return source - image

def reference(rhs, guess, diffusion):
    damping = 0.8
    cells = rhs.shape[1] * rhs.shape[2]
    squares = []
    sources = [rhs]
    fields = []
    field = guess
    for level in range(LEVELS - 1):
        source = sources[level]
        scaled = 2.0 ** level * diffusion
        diag = 1.0 + 4.0 * scaled
        if level == 0:
            field = field + damping * residual(field, source, scaled, diag) / diag
        else:
            field = damping * source / diag
        resid = residual(field, source, scaled, diag)
        squares.append(jnp.sum(resid * resid))
        fields.append(field)
        sources.append(resid[0::2] + resid[1::2])
    level = LEVELS - 1
    source = sources[level]
    scaled = 2.0 ** level * diffusion
    diag = 1.0 + 4.0 * scaled
    field = damping * source / diag
    field = field + damping * residual(field, source, scaled, diag) / diag
    resid = residual(field, source, scaled, diag)
    squares.append(jnp.sum(resid * resid))
    correction = field
    for level in range(LEVELS - 2, -1, -1):
        scaled = 2.0 ** level * diffusion
        diag = 1.0 + 4.0 * scaled
        field = fields[level] + jnp.repeat(correction, 2, axis=0)
        field = field + damping * residual(field, sources[level], scaled, diag) / diag
        correction = field
    scaled = 1.0 * diffusion
    diag = 1.0 + 4.0 * scaled
    resid = residual(correction, rhs, scaled, diag)
    squares.append(jnp.sum(resid * resid))
    norms = jnp.sqrt(jnp.stack(squares) / cells)
    return (correction, norms)
```

```python
import functools

import jax
import jax.numpy as jnp
from jax import lax
from jax.experimental import pallas as pl
from jax.experimental.pallas import tpu as pltpu
from jax.sharding import PartitionSpec as P

LEVELS = 5


damping = 0.8


def with_halo(block, sides, width):
    for axis, dim in sides:
        count = lax.axis_size(axis)
        forward = [(i, i + 1) for i in range(count - 1)]
        backward = [(target, source) for source, target in forward]
        low = lax.ppermute(
            lax.slice_in_dim(block, block.shape[dim] - width, None, axis=dim), axis, forward
        )
        high = lax.ppermute(lax.slice_in_dim(block, 0, width, axis=dim), axis, backward)
        block = jnp.concatenate([low, block, high], axis=dim)
    return block


def shifted(value, axis, steps):
    count = lax.axis_size(axis)
    first, last = (max(0, -steps), min(count, count - steps))
    return lax.ppermute(value, axis, [(source, source + steps) for source in range(first, last)])


def from_partner(value, axis, apart):
    mask = 2**apart
    pairs = [(source, source ^ mask) for source in range(lax.axis_size(axis))]
    return lax.ppermute(value, axis, pairs)


def neighbours(field):
    rows = with_halo(field, (("space", 1),), 1)
    padded = jnp.pad(rows, ((0, 0), (0, 0), (1, 1)))
    total = padded[:, 2:, 1:-1] + padded[:, :-2, 1:-1]
    total = total + padded[:, 1:-1, 2:] + padded[:, 1:-1, :-2]
    return total


def residual(field, source, scaled, diag, stride):
    earlier = shifted(field[-1:], "tm", stride)
    before = jnp.concatenate([earlier, field[:-1]], axis=0)
    image = diag * field - scaled * neighbours(field) - before
    return source - image


def stride_of(level):
    if level == 0:
        return 1
    return 2 ** (level - 1)


def body(rhs, guess, diffusion):
    position = lax.axis_index("tm")
    cells = rhs.shape[1] * lax.axis_size("space") * rhs.shape[2]
    partials = []

    def weight_of(level):
        if level <= 1:
            return jnp.float32(1.0)
        stride = stride_of(level)
        return jnp.where(position % stride == stride - 1, 1.0, 0.0).astype(jnp.float32)

    def record(resid, level):
        local_part = jnp.sum(resid * resid) * weight_of(level)
        partials.append(local_part)

    sources = [rhs]
    fields = []
    field = guess
    for level in range(LEVELS - 1):
        source = sources[level]
        scaled = 2.0**level * diffusion
        diag = 1.0 + 4.0 * scaled
        stride = stride_of(level)
        if level == 0:
            field = field + damping * residual(field, source, scaled, diag, stride) / diag
        else:
            field = damping * source / diag
        resid = residual(field, source, scaled, diag, stride)
        record(resid, level)
        fields.append(field)
        if level == 0:
            coarse = resid[0:1] + resid[1:2]
        else:
            coarse = resid + from_partner(resid, "tm", level - 1)
        sources.append(coarse)
    level = LEVELS - 1
    source = sources[level]
    scaled = 2.0**level * diffusion
    diag = 1.0 + 4.0 * scaled
    stride = stride_of(level)
    field = damping * source / diag
    field = field + damping * residual(field, source, scaled, diag, stride) / diag
    resid = residual(field, source, scaled, diag, stride)
    record(resid, level)
    correction = field
    for level in range(LEVELS - 2, -1, -1):
        scaled = 2.0**level * diffusion
        diag = 1.0 + 4.0 * scaled
        stride = stride_of(level)
        field = fields[level] + correction
        field = field + damping * residual(field, sources[level], scaled, diag, stride) / diag
        correction = field
    scaled = 1.0 * diffusion
    diag = 1.0 + 4.0 * scaled
    resid = residual(correction, rhs, scaled, diag, 1)
    record(resid, 0)
    totals = lax.psum(jnp.stack(partials), ("tm", "space"))
    norms = jnp.sqrt(totals / cells)
    return (correction, norms)


DEVICE = pl.DeviceIdType.MESH
TILE = 8
EDGE = 2 * TILE


def cycle_kernel(
    strips, devices, cells,
    rhs_in, guess_in, diff_in, out, norms_out,
    rhs, guess, diff, v0, g1, v1, r1, v1f, sol, guess_e, v0_e, v1_e, v1f_e, sol_e,
    pair, g2h, v2, c_g2, c_v2, c_g3, c_v3, c_g4, c_v4, c_v4b, acc, tile, gathered, gathered_z,
    load_sem, store_sem, zs_sem, zr_sem, ts_sem, tr_sem, ps_sem, pr_sem, as_sem, ar_sem, al_sem,
    bs_sem, br_sem, bl_sem, ns_sem, nr_sem, ms_sem, mr_sem,
):
    me = lax.axis_index("tm")
    strip = lax.axis_index("space")
    rows, width = rhs_in.shape[1], rhs_in.shape[2]
    chips = devices // 2
    core = lax.rem(me, 2)
    chip = me // 2
    low, high = EDGE, EDGE + rows
    first, last = me == 0, me == devices - 1
    top, bottom = strip == 0, strip == strips - 1
    piece = rows // devices

    def aligned(value):
        return pl.multiple_of(value, TILE)

    def tm_copy(src, dst, send, recv, target):
        return pltpu.make_async_remote_copy(
            src_ref=src, dst_ref=dst, send_sem=send, recv_sem=recv,
            device_id={"tm": target, "space": strip}, device_id_type=DEVICE,
        )

    def space_copy(src, dst, send, recv, target):
        return pltpu.make_async_remote_copy(
            src_ref=src, dst_ref=dst, send_sem=send, recv_sem=recv,
            device_id={"tm": me, "space": target}, device_id_type=DEVICE,
        )

    later = jnp.minimum(me + 1, devices - 1)
    loads = [
        pltpu.make_async_copy(guess_in, guess.at[:, low:high], load_sem.at[0]),
        pltpu.make_async_copy(diff_in, diff.at[low:high], load_sem.at[1]),
        pltpu.make_async_copy(rhs_in, rhs.at[:, low:high], load_sem.at[2]),
    ]
    for copy in loads:
        copy.start()

    barrier = pltpu.get_barrier_semaphore()
    for i in range(1, devices):
        pl.semaphore_signal(
            barrier, inc=1, device_id={"tm": lax.rem(me + i, devices), "space": strip}, device_id_type=DEVICE
        )
    for i in range(1, strips):
        pl.semaphore_signal(
            barrier, inc=1, device_id={"tm": me, "space": lax.rem(strip + i, strips)}, device_id_type=DEVICE
        )
    pl.semaphore_wait(barrier, devices + strips - 2)

    down = jnp.minimum(strip + 1, strips - 1)
    up = jnp.maximum(strip - 1, 0)

    def halo_pair(index, tail, head, low_dst, high_dst):
        return (
            space_copy(tail, low_dst, zs_sem.at[index, 0], zr_sem.at[index, 0], down),
            space_copy(head, high_dst, zs_sem.at[index, 1], zr_sem.at[index, 1], up),
        )

    before_low, after_high = slice(low - TILE, low), slice(high, high + TILE)
    halos = [
        halo_pair(
            0, guess_in.at[:, rows - TILE:rows], guess_in.at[:, 0:TILE],
            guess.at[:, before_low], guess.at[:, after_high],
        ),
        halo_pair(
            1, diff_in.at[rows - TILE:rows], diff_in.at[0:TILE], diff.at[before_low], diff.at[after_high],
        ),
        halo_pair(
            2, rhs_in.at[:, rows - TILE:rows], rhs_in.at[:, 0:TILE],
            rhs.at[:, before_low], rhs.at[:, after_high],
        ),
    ]

    def start_halo(pair_of):
        @pl.when(jnp.logical_not(bottom))
        def _():
            pair_of[0].start()

        @pl.when(jnp.logical_not(top))
        def _():
            pair_of[1].start()

    def finish_halo(pair_of):
        @pl.when(jnp.logical_not(top))
        def _():
            pair_of[0].wait_recv()
            pair_of[1].wait_send()

        @pl.when(jnp.logical_not(bottom))
        def _():
            pair_of[1].wait_recv()
            pair_of[0].wait_send()

    for pair_of in halos:
        start_halo(pair_of)

    half = rows // 2
    quarter = rows // 4
    whole = [
        (low - TILE, quarter), (low - TILE + quarter, quarter + TILE),
        (low + 2 * quarter, quarter), (low + 3 * quarter, quarter + TILE),
    ]
    inner = [(low + quarter * j, quarter) for j in range(4)]
    guess_parts = [(low, half), (low + half, half), (low - TILE, TILE), (high, TILE)]

    def shift(stage, source, target, parts):
        return [
            tm_copy(
                source(start, size), target.at[start:start + size],
                ts_sem.at[stage, j], tr_sem.at[stage, j], later,
            )
            for j, (start, size) in enumerate(parts)
        ]

    def send(copy):
        @pl.when(jnp.logical_not(last))
        def _():
            copy.start()

    def receive(copy):
        @pl.when(jnp.logical_not(first))
        def _():
            copy.wait_recv()

    guess_shift = shift(
        0,
        lambda start, size: (
            guess.at[1, start:start + size] if size == TILE else guess_in.at[1, start - low:start - low + size]
        ),
        guess_e, guess_parts,
    )
    v0_shift = shift(1, lambda start, size: v0.at[1, start:start + size], v0_e, whole)
    v1_shift = shift(2, lambda start, size: v1.at[start:start + size], v1_e, whole)
    v1f_shift = shift(3, lambda start, size: v1f.at[start:start + size], v1f_e, whole)
    sol_shift = shift(4, lambda start, size: sol.at[1, start:start + size], sol_e, inner)
    send(guess_shift[0])
    send(guess_shift[1])

    def blocks(start, size, step, init=None):
        def run(i, carry):
            return step(aligned(start + i * TILE), carry)

        return lax.fori_loop(0, size // TILE, run, init)

    @pl.when(first)
    def _():
        def clear(r, carry):
            zero = jnp.zeros((TILE, width), jnp.float32)
            for ref in (guess_e, v0_e, v1_e, v1f_e, sol_e):
                ref[pl.ds(r, TILE), :] = zero
            v2[1, pl.ds(r, TILE), :] = zero
            return carry

        blocks(low - TILE, rows + 2 * TILE, clear, 0)

    def clear_edge(start):
        for ref in (guess, rhs):
            for p in range(2):
                ref[p, start:start + TILE, :] = jnp.zeros((TILE, width), jnp.float32)
        for p in range(2):
            v2[p, start:start + TILE, :] = jnp.zeros((TILE, width), jnp.float32)
        diff[start:start + TILE, :] = jnp.zeros((TILE, width), jnp.float32)

    @pl.when(top)
    def _():
        clear_edge(low - TILE)

    @pl.when(bottom)
    def _():
        clear_edge(high)

    lane = lax.broadcasted_iota(jnp.int32, (TILE, width), 1)
    not_left, not_right = lane != 0, lane != width - 1

    def stencil(tall):
        mid = tall[TILE:2 * TILE]
        total = tall[TILE - 1:2 * TILE - 1] + tall[TILE + 1:2 * TILE + 1]
        total = total + jnp.where(not_left, pltpu.roll(mid, 1, 1), 0.0)
        total = total + jnp.where(not_right, pltpu.roll(mid, width - 1, 1), 0.0)
        return mid, total

    def tall_at(r):
        return pl.ds(aligned(r - TILE), 3 * TILE)

    def at(r):
        return pl.ds(r, TILE)

    def coefficients(level, r):
        scaled = 2.0**level * diff[at(r), :]
        diag = 1.0 + 4.0 * scaled
        return scaled, diag, damping / diag

    def squares(value, keep=None):
        square = value * value
        if keep is not None:
            square = jnp.where(keep, square, 0.0)
        total = square[:, 0:128]
        for i in range(1, width // 128):
            total = total + square[:, i * 128:(i + 1) * 128]
        return total

    zero_tile = jnp.zeros((TILE, 128), jnp.float32)
    keep_share = 1.0 - damping

    loads[0].wait()
    loads[1].wait()
    finish_halo(halos[0])
    finish_halo(halos[1])
    send(guess_shift[2])
    send(guess_shift[3])
    loads[2].wait()
    finish_halo(halos[2])

    def sweep_last(r, carry):
        scaled, _, weight = coefficients(0, r)
        mid, total = stencil(guess[1, tall_at(r), :])
        v0[1, at(r), :] = keep_share * mid + weight * (rhs[1, at(r), :] + scaled * total + guess[0, at(r), :])
        return carry

    for (start, size), copy in zip(whole, v0_shift):
        blocks(start, size, sweep_last, 0)
        send(copy)

    def sweep_first(r, carry):
        scaled, _, weight = coefficients(0, r)
        mid, total = stencil(guess[0, tall_at(r), :])
        v0[0, at(r), :] = keep_share * mid + weight * (rhs[0, at(r), :] + scaled * total + guess_e[at(r), :])
        return carry

    for copy in guess_shift:
        receive(copy)
    blocks(low - TILE, rows + 2 * TILE, sweep_first, 0)

    def descend(r, carry):
        keep = jnp.logical_and(r >= low, r < high)
        scaled, diag, _ = coefficients(0, r)
        mid, total = stencil(v0[0, tall_at(r), :])
        one = rhs[0, at(r), :] - diag * mid + scaled * total + v0_e[at(r), :]
        late, total = stencil(v0[1, tall_at(r), :])
        two = rhs[1, at(r), :] - diag * late + scaled * total + mid
        source = one + two
        g1[at(r), :] = source
        _, _, weight = coefficients(1, r)
        v1[at(r), :] = weight * source
        return carry + squares(one, keep) + squares(two, keep)

    total0 = zero_tile
    for (start, size), arrived, copy in zip(whole, v0_shift, v1_shift):
        receive(arrived)
        total0 = blocks(start, size, descend, total0)
        send(copy)

    def residual1(r, carry):
        keep = jnp.logical_and(r >= low, r < high)
        scaled, _, _ = coefficients(1, r)
        _, total = stencil(v1[tall_at(r), :])
        resid = keep_share * g1[at(r), :] + scaled * total + v1_e[at(r), :]
        r1[at(r), :] = resid
        return carry + squares(resid, keep)

    total1 = zero_tile
    for (start, size), arrived in zip(whole, v1_shift):
        receive(arrived)
        total1 = blocks(start, size, residual1, total1)

    mine = aligned(low - TILE + core * half)
    theirs = aligned(low - TILE + (1 - core) * half)
    span = half + 2 * TILE
    swap = tm_copy(
        r1.at[pl.ds(theirs, span)], pair.at[pl.ds(theirs, span)], ps_sem, pr_sem, me + 1 - 2 * core
    )
    swap.start()
    swap_in = tm_copy(r1.at[pl.ds(mine, span)], pair.at[pl.ds(mine, span)], ps_sem, pr_sem, me + 1 - 2 * core)
    swap_in.wait_recv()

    def join(r, carry):
        g2h[at(r), :] = r1[at(r), :] + pair[at(r), :]
        return carry

    blocks(mine, span, join, 0)
    tall_piece = piece + 2 * TILE
    c_low, c_high = EDGE, EDGE + piece
    c_rows = slice(c_low - TILE, c_high + TILE)
    for i in range(chips):
        owner = core * chips + i
        src = g2h.at[pl.ds(aligned(low - TILE + owner * piece), tall_piece)]
        copy = tm_copy(src, c_g2.at[chip, c_rows], as_sem.at[i], ar_sem.at[chip], owner)
        local = pltpu.make_async_copy(src, c_g2.at[chip, c_rows], al_sem)

        @pl.when(owner == me)
        def _():
            local.start()
            local.wait()

        @pl.when(owner != me)
        def _():
            copy.start()

    giver = me // chips
    for c in range(chips):
        copy = tm_copy(
            g2h.at[pl.ds(low, tall_piece)], c_g2.at[c, c_rows], as_sem.at[0], ar_sem.at[c],
            lax.rem(me + 1, devices),
        )

        @pl.when(2 * c + giver != me)
        def _():
            copy.wait_recv()

    offset = me * piece

    def coarse_coefficients(level, r):
        return coefficients(level, aligned(r + offset))

    def coarse(step, init=0):
        return blocks(c_low - TILE, tall_piece, step, init)

    def first_sweep(level, source, field, count):
        def step(r, carry):
            _, _, weight = coarse_coefficients(level, r)
            for p in range(count):
                field[p, at(r), :] = weight * source[p, at(r), :]
            return carry

        coarse(step)

    def coarse_residual(level, source, field, target, count):
        def step(r, carry):
            keep = jnp.logical_and(r >= c_low, r < c_high)
            scaled, _, _ = coarse_coefficients(level, r)
            earlier, even = None, None
            for p in range(count):
                mid, total = stencil(field[p, tall_at(r), :])
                resid = keep_share * source[p, at(r), :] + scaled * total
                if p:
                    resid = resid + earlier
                earlier = mid
                carry = carry + squares(resid, keep)
                if p % 2 == 0:
                    even = resid
                else:
                    target[p // 2, at(r), :] = even + resid
            return carry

        return coarse(step, zero_tile)

    def ascend(level, source, field, above, target, count):
        def step(r, carry):
            scaled, _, weight = coarse_coefficients(level, r)
            earlier = None
            for p in range(count):
                mid, total = stencil(field[p, tall_at(r), :] + above[p // 2, tall_at(r), :])
                value = source[p, at(r), :] + scaled * total
                if p:
                    value = value + earlier
                earlier = mid
                target[p, at(r), :] = keep_share * mid + weight * value
            return carry

        coarse(step)

    points2, points3 = chips, chips // 2
    first_sweep(2, c_g2, c_v2, points2)
    total2 = coarse_residual(2, c_g2, c_v2, c_g3, points2)
    first_sweep(3, c_g3, c_v3, points3)
    total3 = coarse_residual(3, c_g3, c_v3, c_g4, points3)
    first_sweep(4, c_g4, c_v4, 1)

    def second_sweep(r, carry):
        scaled, _, weight = coarse_coefficients(4, r)
        mid, total = stencil(c_v4[0, tall_at(r), :])
        c_v4b[0, at(r), :] = keep_share * mid + weight * (c_g4[0, at(r), :] + scaled * total)
        return carry

    coarse(second_sweep)

    def residual4(r, carry):
        scaled, diag, _ = coarse_coefficients(4, r)
        mid, total = stencil(c_v4b[0, tall_at(r), :])
        return carry + squares(c_g4[0, at(r), :] - diag * mid + scaled * total)

    total4 = blocks(c_low, piece, residual4, zero_tile)
    c_v3f, c_v2f = acc
    ascend(3, c_g3, c_v3, c_v4b, c_v3f, points3)
    ascend(2, c_g2, c_v2, c_v3f, c_v2f, points2)

    back = []
    place = pl.ds(aligned(low + offset), piece)
    for j in range(devices):
        wants = [(0, j // 2)]
        if j % 2 == 0 and j > 0:
            wants.append((1, j // 2 - 1))
        for kind, point in wants:
            src, dst = c_v2f.at[point, c_low:c_high], v2.at[kind, place]
            copy = tm_copy(src, dst, bs_sem.at[kind, j], br_sem.at[kind, me], j)
            local = pltpu.make_async_copy(src, dst, bl_sem.at[kind])
            back.append((j, copy))

            @pl.when(me == j)
            def _():
                local.start()
                local.wait()

            @pl.when(me != j)
            def _():
                copy.start()

    has_second = jnp.logical_and(core == 0, jnp.logical_not(first))
    for kind in range(2):
        for k in range(devices):
            copy = tm_copy(
                c_v2f.at[0, c_low:c_high], v2.at[kind, low + k * piece:low + (k + 1) * piece],
                bs_sem.at[kind, 0], br_sem.at[kind, k], lax.rem(me + 1, devices),
            )
            needed = me != k
            if kind:
                needed = jnp.logical_and(needed, has_second)

            @pl.when(needed)
            def _():
                copy.wait_recv()

    v2_halos = [
        halo_pair(
            3 + kind, v2.at[kind, high - TILE:high], v2.at[kind, low:low + TILE],
            v2.at[kind, before_low], v2.at[kind, after_high],
        )
        for kind in range(2)
    ]
    start_halo(v2_halos[0])

    @pl.when(has_second)
    def _():
        start_halo(v2_halos[1])

    finish_halo(v2_halos[0])

    @pl.when(has_second)
    def _():
        finish_halo(v2_halos[1])

    kind = 1 - core

    def ascend1(r, carry):
        scaled, _, weight = coefficients(1, r)
        mid, total = stencil(v1[tall_at(r), :] + v2[0, tall_at(r), :])
        earlier = v1_e[at(r), :] + v2[kind, at(r), :]
        v1f[at(r), :] = keep_share * mid + weight * (g1[at(r), :] + scaled * total + earlier)
        return carry

    for (start, size), copy in zip(whole, v1f_shift):
        blocks(start, size, ascend1, 0)
        send(copy)

    def ascend_last(r, carry):
        scaled, _, weight = coefficients(0, r)
        mid, total = stencil(v0[1, tall_at(r), :] + v1f[tall_at(r), :])
        earlier = v0[0, at(r), :] + v1f[at(r), :]
        sol[1, at(r), :] = keep_share * mid + weight * (rhs[1, at(r), :] + scaled * total + earlier)
        return carry

    blocks(low - TILE, TILE, ascend_last, 0)
    for (start, size), copy in zip(inner, sol_shift):
        blocks(start, size, ascend_last, 0)
        send(copy)
    blocks(high, TILE, ascend_last, 0)

    def ascend_first(r, carry):
        scaled, _, weight = coefficients(0, r)
        mid, total = stencil(v0[0, tall_at(r), :] + v1f[tall_at(r), :])
        earlier = v0_e[at(r), :] + v1f_e[at(r), :]
        sol[0, at(r), :] = keep_share * mid + weight * (rhs[0, at(r), :] + scaled * total + earlier)
        return carry

    for (start, size), arrived in zip(whole, v1f_shift):
        receive(arrived)
        blocks(start, size, ascend_first, 0)
    stores = pltpu.make_async_copy(sol.at[:, low:high], out, store_sem)
    stores.start()

    def final_last(r, carry):
        scaled, diag, _ = coefficients(0, r)
        mid, total = stencil(sol[1, tall_at(r), :])
        return carry + squares(rhs[1, at(r), :] - diag * mid + scaled * total + sol[0, at(r), :])

    total5 = blocks(low, rows, final_last, zero_tile)

    def final_first(r, carry):
        scaled, diag, _ = coefficients(0, r)
        mid, total = stencil(sol[0, tall_at(r), :])
        return carry + squares(rhs[0, at(r), :] - diag * mid + scaled * total + sol_e[at(r), :])

    for (start, size), arrived in zip(inner, sol_shift):
        receive(arrived)
        total5 = blocks(start, size, final_first, total5)

    parts = [total0, total1, total2, total3, total4, total5]
    for level, value in enumerate(parts):
        tile[level:level + 1, :] = jnp.sum(value, axis=0, keepdims=True)
    for level in range(len(parts), TILE):
        tile[level:level + 1, :] = jnp.zeros((1, 128), jnp.float32)

    def exchange(count, own, source, slots, copier, send_sems, recv_sems):
        slots[pl.ds(own, 1)] = source[...][None]
        sent = [
            copier(source, slots.at[own], send_sems.at[i], recv_sems.at[own], lax.rem(own + i, count))
            for i in range(1, count)
        ]
        for copy in sent:
            copy.start()
        for i in range(1, count):
            other = lax.rem(own + i, count)
            copier(source, slots.at[other], send_sems.at[i], recv_sems.at[other], other).wait_recv()
        for copy in sent:
            copy.wait_send()
        total = slots[0]
        for i in range(1, count):
            total = total + slots[i]
        return total

    total = exchange(devices, me, tile, gathered, tm_copy, ns_sem, nr_sem)
    tile[...] = total
    total = exchange(strips, strip, tile, gathered_z, space_copy, ms_sem, mr_sem)
    summed = jnp.sum(total, axis=1, keepdims=True)
    norms_out[...] = jnp.broadcast_to(jnp.sqrt(summed * (1.0 / cells)), (TILE, 128))

    stores.wait()
    for group in (guess_shift, v0_shift, v1_shift, v1f_shift, sol_shift):
        for copy in group:
            @pl.when(jnp.logical_not(last))
            def _():
                copy.wait_send()
    swap.wait_send()
    for i in range(chips):
        owner = core * chips + i
        copy = tm_copy(
            g2h.at[pl.ds(aligned(low - TILE + owner * piece), tall_piece)], c_g2.at[chip, c_rows],
            as_sem.at[i], ar_sem.at[chip], owner,
        )

        @pl.when(owner != me)
        def _():
            copy.wait_send()
    for j, copy in back:
        @pl.when(me != j)
        def _():
            copy.wait_send()


def fast_body(rhs, guess, diffusion):
    devices, strips = lax.axis_size("tm"), lax.axis_size("space")
    rows, width = rhs.shape[1:]
    chips = devices // 2
    cells = rows * strips * width
    height = rows + 2 * EDGE
    c_height = rows // devices + 2 * EDGE

    def plane(*lead):
        return pltpu.VMEM(lead + (height, width), jnp.float32)

    def coarse(count):
        return pltpu.VMEM((count, c_height, width), jnp.float32)

    dma = pltpu.SemaphoreType.DMA
    scratch = [
        plane(2), plane(2), plane(), plane(2), plane(), plane(), plane(), plane(), plane(2),
        plane(), plane(), plane(), plane(), plane(),
        plane(), plane(), plane(2),
        coarse(chips), coarse(chips), coarse(chips // 2), coarse(chips // 2), coarse(1), coarse(1), coarse(1),
        (coarse(chips // 2), coarse(chips)),
        pltpu.VMEM((TILE, 128), jnp.float32),
        pltpu.VMEM((devices, TILE, 128), jnp.float32),
        pltpu.VMEM((strips, TILE, 128), jnp.float32),
        dma((3,)), dma, dma((5, 2)), dma((5, 2)), dma((5, 4)), dma((5, 4)), dma, dma,
        dma((chips,)), dma((chips,)), dma, dma((2, devices)), dma((2, devices)), dma((2,)),
        dma((devices,)), dma((devices,)), dma((strips,)), dma((strips,)),
    ]
    any_space = pl.BlockSpec(memory_space=pl.ANY)
    result, norms = pl.pallas_call(
        functools.partial(cycle_kernel, strips, devices, cells),
        out_shape=(
            jax.ShapeDtypeStruct(rhs.shape, jnp.float32),
            jax.ShapeDtypeStruct((TILE, 128), jnp.float32),
        ),
        in_specs=[any_space] * 3,
        out_specs=(any_space, pl.BlockSpec(memory_space=pltpu.VMEM)),
        scratch_shapes=scratch,
        compiler_params=pltpu.CompilerParams(
            collective_id=0, has_side_effects=True, vmem_limit_bytes=60 * 2**20
        ),
    )(rhs, guess, diffusion)
    return result, norms[:LEVELS + 1, 0]


def solution(mesh):
    in_specs = (P("tm", "space", None), P("tm", "space", None), P("space", None))
    out_specs = (P("tm", "space", None), P())

    def choose(rhs, guess, diffusion):
        points = rhs.shape[0] * lax.axis_size("tm")
        one_coarsest = points == 2 ** (LEVELS - 1) and rhs.shape[0] == 2
        even = rhs.shape[1] % (TILE * lax.axis_size("tm")) == 0 and rhs.shape[2] % 128 == 0
        if one_coarsest and even:
            return fast_body(rhs, guess, diffusion)
        return body(rhs, guess, diffusion)

    return jax.shard_map(choose, mesh=mesh, in_specs=in_specs, out_specs=out_specs, check_vma=False)
```

```python
import functools

import jax
import jax.numpy as jnp
from jax import lax
from jax.experimental import pallas as pl
from jax.experimental.pallas import tpu as pltpu
from jax.sharding import PartitionSpec as P

LEVELS = 5


damping = 0.8


def with_halo(block, sides, width):
    for axis, dim in sides:
        count = lax.axis_size(axis)
        forward = [(i, i + 1) for i in range(count - 1)]
        backward = [(target, source) for source, target in forward]
        low = lax.ppermute(
            lax.slice_in_dim(block, block.shape[dim] - width, None, axis=dim), axis, forward
        )
        high = lax.ppermute(lax.slice_in_dim(block, 0, width, axis=dim), axis, backward)
        block = jnp.concatenate([low, block, high], axis=dim)
    return block


def shifted(value, axis, steps):
    count = lax.axis_size(axis)
    first, last = (max(0, -steps), min(count, count - steps))
    return lax.ppermute(value, axis, [(source, source + steps) for source in range(first, last)])


def from_partner(value, axis, apart):
    mask = 2**apart
    pairs = [(source, source ^ mask) for source in range(lax.axis_size(axis))]
    return lax.ppermute(value, axis, pairs)


def neighbours(field):
    rows = with_halo(field, (("space", 1),), 1)
    padded = jnp.pad(rows, ((0, 0), (0, 0), (1, 1)))
    total = padded[:, 2:, 1:-1] + padded[:, :-2, 1:-1]
    total = total + padded[:, 1:-1, 2:] + padded[:, 1:-1, :-2]
    return total


def residual(field, source, scaled, diag, stride):
    earlier = shifted(field[-1:], "tm", stride)
    before = jnp.concatenate([earlier, field[:-1]], axis=0)
    image = diag * field - scaled * neighbours(field) - before
    return source - image


def stride_of(level):
    if level == 0:
        return 1
    return 2 ** (level - 1)


def body(rhs, guess, diffusion):
    position = lax.axis_index("tm")
    cells = rhs.shape[1] * lax.axis_size("space") * rhs.shape[2]
    partials = []

    def weight_of(level):
        if level <= 1:
            return jnp.float32(1.0)
        stride = stride_of(level)
        return jnp.where(position % stride == stride - 1, 1.0, 0.0).astype(jnp.float32)

    def record(resid, level):
        local_part = jnp.sum(resid * resid) * weight_of(level)
        partials.append(local_part)

    sources = [rhs]
    fields = []
    field = guess
    for level in range(LEVELS - 1):
        source = sources[level]
        scaled = 2.0**level * diffusion
        diag = 1.0 + 4.0 * scaled
        stride = stride_of(level)
        if level == 0:
            field = field + damping * residual(field, source, scaled, diag, stride) / diag
        else:
            field = damping * source / diag
        resid = residual(field, source, scaled, diag, stride)
        record(resid, level)
        fields.append(field)
        if level == 0:
            coarse = resid[0:1] + resid[1:2]
        else:
            coarse = resid + from_partner(resid, "tm", level - 1)
        sources.append(coarse)
    level = LEVELS - 1
    source = sources[level]
    scaled = 2.0**level * diffusion
    diag = 1.0 + 4.0 * scaled
    stride = stride_of(level)
    field = damping * source / diag
    field = field + damping * residual(field, source, scaled, diag, stride) / diag
    resid = residual(field, source, scaled, diag, stride)
    record(resid, level)
    correction = field
    for level in range(LEVELS - 2, -1, -1):
        scaled = 2.0**level * diffusion
        diag = 1.0 + 4.0 * scaled
        stride = stride_of(level)
        field = fields[level] + correction
        field = field + damping * residual(field, sources[level], scaled, diag, stride) / diag
        correction = field
    scaled = 1.0 * diffusion
    diag = 1.0 + 4.0 * scaled
    resid = residual(correction, rhs, scaled, diag, 1)
    record(resid, 0)
    totals = lax.psum(jnp.stack(partials), ("tm", "space"))
    norms = jnp.sqrt(totals / cells)
    return (correction, norms)


DEVICE = pl.DeviceIdType.MESH
TILE = 8
EDGE = 2 * TILE


def cycle_kernel(
    strips, devices, cells,
    rhs_in, guess_in, diff_in, out, norms_out,
    rhs, guess, diff, v0, g1, v1, r1, v1f, sol, guess_e, v0_e, v1_e, v1_ee, v1f_e, sol_e,
    pair, g2h, v2, c_g2, c_v2, c_g3, c_v3, c_g4, c_v4, c_v4b, acc, tile, gathered, gathered_z,
    load_sem, store_sem, zs_sem, zr_sem, ts_sem, tr_sem, ps_sem, pr_sem, as_sem, ar_sem, al_sem,
    bs_sem, br_sem, bl_sem, rs_sem, es_sem, er_sem, ns_sem, nr_sem, ms_sem, mr_sem,
):
    me = lax.axis_index("tm")
    strip = lax.axis_index("space")
    rows, width = rhs_in.shape[1], rhs_in.shape[2]
    chips = devices // 2
    core = lax.rem(me, 2)
    chip = me // 2
    low, high = EDGE, EDGE + rows
    first, last = me == 0, me == devices - 1
    top, bottom = strip == 0, strip == strips - 1
    piece = rows // devices

    def aligned(value):
        return pl.multiple_of(value, TILE)

    def tm_copy(src, dst, send, recv, target):
        return pltpu.make_async_remote_copy(
            src_ref=src, dst_ref=dst, send_sem=send, recv_sem=recv,
            device_id={"tm": target, "space": strip}, device_id_type=DEVICE,
        )

    def space_copy(src, dst, send, recv, target):
        return pltpu.make_async_remote_copy(
            src_ref=src, dst_ref=dst, send_sem=send, recv_sem=recv,
            device_id={"tm": me, "space": target}, device_id_type=DEVICE,
        )

    later = jnp.minimum(me + 1, devices - 1)
    loads = [
        pltpu.make_async_copy(guess_in, guess.at[:, low:high], load_sem.at[0]),
        pltpu.make_async_copy(diff_in, diff.at[low:high], load_sem.at[1]),
        pltpu.make_async_copy(rhs_in, rhs.at[:, low:high], load_sem.at[2]),
    ]
    for copy in loads:
        copy.start()

    barrier = pltpu.get_barrier_semaphore()
    for i in range(1, devices):
        pl.semaphore_signal(
            barrier, inc=1, device_id={"tm": lax.rem(me + i, devices), "space": strip}, device_id_type=DEVICE
        )
    for i in range(1, strips):
        pl.semaphore_signal(
            barrier, inc=1, device_id={"tm": me, "space": lax.rem(strip + i, strips)}, device_id_type=DEVICE
        )
    pl.semaphore_wait(barrier, devices + strips - 2)

    down = jnp.minimum(strip + 1, strips - 1)
    up = jnp.maximum(strip - 1, 0)

    def halo_pair(index, tail, head, low_dst, high_dst):
        return (
            space_copy(tail, low_dst, zs_sem.at[index, 0], zr_sem.at[index, 0], down),
            space_copy(head, high_dst, zs_sem.at[index, 1], zr_sem.at[index, 1], up),
        )

    before_low, after_high = slice(low - TILE, low), slice(high, high + TILE)
    halos = [
        halo_pair(
            0, guess_in.at[:, rows - TILE:rows], guess_in.at[:, 0:TILE],
            guess.at[:, before_low], guess.at[:, after_high],
        ),
        halo_pair(
            1, diff_in.at[rows - TILE:rows], diff_in.at[0:TILE], diff.at[before_low], diff.at[after_high],
        ),
        halo_pair(
            2, rhs_in.at[:, rows - TILE:rows], rhs_in.at[:, 0:TILE],
            rhs.at[:, before_low], rhs.at[:, after_high],
        ),
    ]

    def start_halo(pair_of):
        @pl.when(jnp.logical_not(bottom))
        def _():
            pair_of[0].start()

        @pl.when(jnp.logical_not(top))
        def _():
            pair_of[1].start()

    def finish_halo(pair_of):
        @pl.when(jnp.logical_not(top))
        def _():
            pair_of[0].wait_recv()
            pair_of[1].wait_send()

        @pl.when(jnp.logical_not(bottom))
        def _():
            pair_of[1].wait_recv()
            pair_of[0].wait_send()

    for pair_of in halos:
        start_halo(pair_of)

    half = rows // 2
    quarter = rows // 4
    whole = [
        (low - TILE, quarter), (low - TILE + quarter, quarter + TILE),
        (low + 2 * quarter, quarter), (low + 3 * quarter, quarter + TILE),
    ]
    inner = [(low + quarter * j, quarter) for j in range(4)]
    guess_parts = [(low, half), (low + half, half), (low - TILE, TILE), (high, TILE)]

    def shift(stage, source, target, parts):
        return [
            tm_copy(
                source(start, size), target.at[start:start + size],
                ts_sem.at[stage, j], tr_sem.at[stage, j], later,
            )
            for j, (start, size) in enumerate(parts)
        ]

    def send(copy):
        @pl.when(jnp.logical_not(last))
        def _():
            copy.start()

    def receive(copy):
        @pl.when(jnp.logical_not(first))
        def _():
            copy.wait_recv()

    guess_shift = shift(
        0,
        lambda start, size: (
            guess.at[1, start:start + size] if size == TILE else guess_in.at[1, start - low:start - low + size]
        ),
        guess_e, guess_parts,
    )
    v0_shift = shift(1, lambda start, size: v0.at[1, start:start + size], v0_e, whole)
    v1_shift = shift(2, lambda start, size: v1.at[start:start + size], v1_e, whole)
    v1f_shift = shift(3, lambda start, size: v1f.at[start:start + size], v1f_e, whole)
    sol_shift = shift(4, lambda start, size: sol.at[1, start:start + size], sol_e, inner)
    send(guess_shift[0])
    send(guess_shift[1])

    def blocks(start, size, step, init=None):
        def run(i, carry):
            return step(aligned(start + i * TILE), carry)

        return lax.fori_loop(0, size // TILE, run, init)

    @pl.when(first)
    def _():
        def clear(r, carry):
            zero = jnp.zeros((TILE, width), jnp.float32)
            for ref in (guess_e, v0_e, v1_e, v1_ee, v1f_e, sol_e):
                ref[pl.ds(r, TILE), :] = zero
            v2[1, pl.ds(r, TILE), :] = zero
            return carry

        blocks(low - TILE, rows + 2 * TILE, clear, 0)

    def clear_edge(start):
        for ref in (guess, rhs):
            for p in range(2):
                ref[p, start:start + TILE, :] = jnp.zeros((TILE, width), jnp.float32)
        for p in range(2):
            v2[p, start:start + TILE, :] = jnp.zeros((TILE, width), jnp.float32)
        diff[start:start + TILE, :] = jnp.zeros((TILE, width), jnp.float32)

    @pl.when(top)
    def _():
        clear_edge(low - TILE)

    @pl.when(bottom)
    def _():
        clear_edge(high)

    lane = lax.broadcasted_iota(jnp.int32, (TILE, width), 1)
    not_left, not_right = lane != 0, lane != width - 1

    def stencil(tall):
        mid = tall[TILE:2 * TILE]
        total = tall[TILE - 1:2 * TILE - 1] + tall[TILE + 1:2 * TILE + 1]
        total = total + jnp.where(not_left, pltpu.roll(mid, 1, 1), 0.0)
        total = total + jnp.where(not_right, pltpu.roll(mid, width - 1, 1), 0.0)
        return mid, total

    def tall_at(r):
        return pl.ds(aligned(r - TILE), 3 * TILE)

    def at(r):
        return pl.ds(r, TILE)

    def coefficients(level, r):
        scaled = 2.0**level * diff[at(r), :]
        diag = 1.0 + 4.0 * scaled
        return scaled, diag, damping / diag

    def squares(value, keep=None):
        square = value * value
        if keep is not None:
            square = jnp.where(keep, square, 0.0)
        total = square[:, 0:128]
        for i in range(1, width // 128):
            total = total + square[:, i * 128:(i + 1) * 128]
        return total

    zero_tile = jnp.zeros((TILE, 128), jnp.float32)
    keep_share = 1.0 - damping

    loads[0].wait()
    loads[1].wait()
    finish_halo(halos[0])
    finish_halo(halos[1])
    send(guess_shift[2])
    send(guess_shift[3])
    loads[2].wait()
    finish_halo(halos[2])

    def sweep_last(r, carry):
        scaled, _, weight = coefficients(0, r)
        mid, total = stencil(guess[1, tall_at(r), :])
        v0[1, at(r), :] = keep_share * mid + weight * (rhs[1, at(r), :] + scaled * total + guess[0, at(r), :])
        return carry

    for (start, size), copy in zip(whole, v0_shift):
        blocks(start, size, sweep_last, 0)
        send(copy)

    def sweep_first(r, carry):
        scaled, _, weight = coefficients(0, r)
        mid, total = stencil(guess[0, tall_at(r), :])
        v0[0, at(r), :] = keep_share * mid + weight * (rhs[0, at(r), :] + scaled * total + guess_e[at(r), :])
        return carry

    for copy in guess_shift:
        receive(copy)
    blocks(low - TILE, rows + 2 * TILE, sweep_first, 0)

    def descend(r, carry):
        keep = jnp.logical_and(r >= low, r < high)
        scaled, diag, _ = coefficients(0, r)
        mid, total = stencil(v0[0, tall_at(r), :])
        one = rhs[0, at(r), :] - diag * mid + scaled * total + v0_e[at(r), :]
        late, total = stencil(v0[1, tall_at(r), :])
        two = rhs[1, at(r), :] - diag * late + scaled * total + mid
        source = one + two
        g1[at(r), :] = source
        _, _, weight = coefficients(1, r)
        v1[at(r), :] = weight * source
        return carry + squares(one, keep) + squares(two, keep)

    total0 = zero_tile
    for (start, size), arrived, copy in zip(whole, v0_shift, v1_shift):
        receive(arrived)
        total0 = blocks(start, size, descend, total0)
        send(copy)

    def residual1(r, carry):
        keep = jnp.logical_and(r >= low, r < high)
        scaled, _, _ = coefficients(1, r)
        _, total = stencil(v1[tall_at(r), :])
        resid = keep_share * g1[at(r), :] + scaled * total + v1_e[at(r), :]
        r1[at(r), :] = resid
        return carry + squares(resid, keep)

    total1 = zero_tile
    for (start, size), arrived in zip(whole, v1_shift):
        receive(arrived)
        total1 = blocks(start, size, residual1, total1)

    mine = aligned(low - TILE + core * half)
    theirs = aligned(low - TILE + (1 - core) * half)
    span = half + 2 * TILE
    swap = tm_copy(
        r1.at[pl.ds(theirs, span)], pair.at[pl.ds(theirs, span)], ps_sem, pr_sem, me + 1 - 2 * core
    )
    swap.start()
    swap_in = tm_copy(r1.at[pl.ds(mine, span)], pair.at[pl.ds(mine, span)], ps_sem, pr_sem, me + 1 - 2 * core)
    swap_in.wait_recv()

    def join(r, carry):
        g2h[at(r), :] = r1[at(r), :] + pair[at(r), :]
        return carry

    blocks(mine, span, join, 0)
    tall_piece = piece + 2 * TILE
    c_low, c_high = EDGE, EDGE + piece
    c_rows = slice(c_low - TILE, c_high + TILE)
    for i in range(chips):
        owner = core * chips + i
        src = g2h.at[pl.ds(aligned(low - TILE + owner * piece), tall_piece)]
        copy = tm_copy(src, c_g2.at[chip, c_rows], as_sem.at[i], ar_sem.at[chip], owner)
        local = pltpu.make_async_copy(src, c_g2.at[chip, c_rows], al_sem)

        @pl.when(owner == me)
        def _():
            local.start()
            local.wait()

        @pl.when(owner != me)
        def _():
            copy.start()

    giver = me // chips
    for c in range(chips):
        copy = tm_copy(
            g2h.at[pl.ds(low, tall_piece)], c_g2.at[c, c_rows], as_sem.at[0], ar_sem.at[c],
            lax.rem(me + 1, devices),
        )

        @pl.when(2 * c + giver != me)
        def _():
            copy.wait_recv()

    skip_shift = [
        tm_copy(
            v1.at[start:start + size], v1_ee.at[start:start + size], es_sem.at[j], er_sem.at[j],
            jnp.minimum(me + 2, devices - 1),
        )
        for j, (start, size) in enumerate(whole)
    ]
    sends_skip = jnp.logical_and(core == 0, chip < chips - 1)
    has_second = jnp.logical_and(core == 0, jnp.logical_not(first))

    @pl.when(sends_skip)
    def _():
        for copy in skip_shift:
            copy.start()

    offset = me * piece

    def coarse_coefficients(level, r):
        return coefficients(level, aligned(r + offset))

    def coarse(step, init=0):
        return blocks(c_low - TILE, tall_piece, step, init)

    def first_sweep(level, source, field, count):
        def step(r, carry):
            _, _, weight = coarse_coefficients(level, r)
            for p in range(count):
                field[p, at(r), :] = weight * source[p, at(r), :]
            return carry

        coarse(step)

    def coarse_residual(level, source, field, target, count):
        def step(r, carry):
            keep = jnp.logical_and(r >= c_low, r < c_high)
            scaled, _, _ = coarse_coefficients(level, r)
            earlier, even = None, None
            for p in range(count):
                mid, total = stencil(field[p, tall_at(r), :])
                resid = keep_share * source[p, at(r), :] + scaled * total
                if p:
                    resid = resid + earlier
                earlier = mid
                carry = carry + squares(resid, keep)
                if p % 2 == 0:
                    even = resid
                else:
                    target[p // 2, at(r), :] = even + resid
            return carry

        return coarse(step, zero_tile)

    def ascend(level, source, field, above, target, count):
        def step(r, carry):
            scaled, _, weight = coarse_coefficients(level, r)
            earlier = None
            for p in range(count):
                mid, total = stencil(field[p, tall_at(r), :] + above[p // 2, tall_at(r), :])
                value = source[p, at(r), :] + scaled * total
                if p:
                    value = value + earlier
                earlier = mid
                target[p, at(r), :] = keep_share * mid + weight * value
            return carry

        coarse(step)

    points2, points3 = chips, chips // 2
    first_sweep(2, c_g2, c_v2, points2)
    total2 = coarse_residual(2, c_g2, c_v2, c_g3, points2)
    first_sweep(3, c_g3, c_v3, points3)
    total3 = coarse_residual(3, c_g3, c_v3, c_g4, points3)
    first_sweep(4, c_g4, c_v4, 1)

    def second_sweep(r, carry):
        scaled, _, weight = coarse_coefficients(4, r)
        mid, total = stencil(c_v4[0, tall_at(r), :])
        c_v4b[0, at(r), :] = keep_share * mid + weight * (c_g4[0, at(r), :] + scaled * total)
        return carry

    coarse(second_sweep)

    def residual4(r, carry):
        scaled, diag, _ = coarse_coefficients(4, r)
        mid, total = stencil(c_v4b[0, tall_at(r), :])
        return carry + squares(c_g4[0, at(r), :] - diag * mid + scaled * total)

    total4 = blocks(c_low, piece, residual4, zero_tile)
    c_v3f, c_v2f = acc
    ascend(3, c_g3, c_v3, c_v4b, c_v3f, points3)
    ascend(2, c_g2, c_v2, c_v3f, c_v2f, points2)

    back = []
    place = pl.ds(aligned(low + offset), piece)
    for c in range(chips):
        wants = [(0, 2 * c + core, c)]
        if c > 0:
            wants.append((1, 2 * c, c - 1))
        for kind, target, point in wants:
            src, dst = c_v2f.at[point, c_low:c_high], v2.at[kind, place]
            copy = tm_copy(src, dst, bs_sem.at[kind, c], br_sem.at[kind, me], target)
            local = pltpu.make_async_copy(src, dst, bl_sem.at[kind])
            back.append((target, copy))

            @pl.when(me == target)
            def _():
                local.start()
                local.wait()

            @pl.when(me != target)
            def _():
                copy.start()

    sibling = me + 1 - 2 * core
    relays = []
    for i in range(chips):
        for side in (core, 1 - core):
            k = 2 * i + side
            rows_of = pl.ds(aligned(low + k * piece), piece)
            arrival = tm_copy(v2.at[0, rows_of], v2.at[0, rows_of], rs_sem.at[i], br_sem.at[0, k], sibling)
            relays.append((k, arrival))
    for k, arrival in relays[0::2]:
        @pl.when(k != me)
        def _():
            arrival.wait_recv()

        arrival.start()
    for k, arrival in relays[1::2]:
        arrival.wait_recv()
    for k in range(devices):
        rows_of = slice(low + k * piece, low + (k + 1) * piece)
        arrival = tm_copy(v2.at[1, rows_of], v2.at[1, rows_of], bs_sem.at[1, 0], br_sem.at[1, k], sibling)

        @pl.when(jnp.logical_and(k != me, has_second))
        def _():
            arrival.wait_recv()

    v2_halos = [
        halo_pair(
            3 + kind, v2.at[kind, high - TILE:high], v2.at[kind, low:low + TILE],
            v2.at[kind, before_low], v2.at[kind, after_high],
        )
        for kind in range(2)
    ]
    start_halo(v2_halos[0])

    @pl.when(has_second)
    def _():
        start_halo(v2_halos[1])

    finish_halo(v2_halos[0])

    @pl.when(has_second)
    def _():
        finish_halo(v2_halos[1])

    kind = 1 - core

    def ascend1(r, carry):
        scaled, _, weight = coefficients(1, r)
        mid, total = stencil(v1[tall_at(r), :] + v2[0, tall_at(r), :])
        earlier = v1_e[at(r), :] + v2[kind, at(r), :]
        v1f[at(r), :] = keep_share * mid + weight * (g1[at(r), :] + scaled * total + earlier)
        return carry

    for (start, size), copy in zip(whole, v1f_shift):
        blocks(start, size, ascend1, 0)

        @pl.when(core == 0)
        def _():
            copy.start()

    def ascend_last(r, carry):
        scaled, _, weight = coefficients(0, r)
        mid, total = stencil(v0[1, tall_at(r), :] + v1f[tall_at(r), :])
        earlier = v0[0, at(r), :] + v1f[at(r), :]
        sol[1, at(r), :] = keep_share * mid + weight * (rhs[1, at(r), :] + scaled * total + earlier)
        return carry

    blocks(low - TILE, TILE, ascend_last, 0)
    for (start, size), copy in zip(inner, sol_shift):
        blocks(start, size, ascend_last, 0)
        send(copy)
    blocks(high, TILE, ascend_last, 0)

    def ascend_first(r, carry):
        scaled, _, weight = coefficients(0, r)
        mid, total = stencil(v0[0, tall_at(r), :] + v1f[tall_at(r), :])
        earlier = v0_e[at(r), :] + v1f_e[at(r), :]
        sol[0, at(r), :] = keep_share * mid + weight * (rhs[0, at(r), :] + scaled * total + earlier)
        return carry

    def ascend_before(r, carry):
        scaled, _, weight = coefficients(1, r)
        early, above = v1_e[at(r), :], v2[1, at(r), :]
        mid, total = stencil(v1_e[tall_at(r), :] + v2[1, tall_at(r), :])
        v1f_e[at(r), :] = keep_share * mid + early + weight * (scaled * total + v1_ee[at(r), :] + above)
        return carry

    for (start, size), arrived, skipped in zip(whole, v1f_shift, skip_shift):
        @pl.when(core == 1)
        def _():
            arrived.wait_recv()

        @pl.when(has_second)
        def _():
            skipped.wait_recv()
            blocks(start, size, ascend_before, 0)

        blocks(start, size, ascend_first, 0)
    stores = pltpu.make_async_copy(sol.at[:, low:high], out, store_sem)
    stores.start()

    def final_last(r, carry):
        scaled, diag, _ = coefficients(0, r)
        mid, total = stencil(sol[1, tall_at(r), :])
        return carry + squares(rhs[1, at(r), :] - diag * mid + scaled * total + sol[0, at(r), :])

    total5 = blocks(low, rows, final_last, zero_tile)

    def final_first(r, carry):
        scaled, diag, _ = coefficients(0, r)
        mid, total = stencil(sol[0, tall_at(r), :])
        return carry + squares(rhs[0, at(r), :] - diag * mid + scaled * total + sol_e[at(r), :])

    for (start, size), arrived in zip(inner, sol_shift):
        receive(arrived)
        total5 = blocks(start, size, final_first, total5)

    parts = [total0, total1, total2, total3, total4, total5]
    for level, value in enumerate(parts):
        tile[level:level + 1, :] = jnp.sum(value, axis=0, keepdims=True)
    for level in range(len(parts), TILE):
        tile[level:level + 1, :] = jnp.zeros((1, 128), jnp.float32)

    def exchange(count, own, source, slots, copier, send_sems, recv_sems):
        slots[pl.ds(own, 1)] = source[...][None]
        sent = [
            copier(source, slots.at[own], send_sems.at[i], recv_sems.at[own], lax.rem(own + i, count))
            for i in range(1, count)
        ]
        for copy in sent:
            copy.start()
        for i in range(1, count):
            other = lax.rem(own + i, count)
            copier(source, slots.at[other], send_sems.at[i], recv_sems.at[other], other).wait_recv()
        for copy in sent:
            copy.wait_send()
        total = slots[0]
        for i in range(1, count):
            total = total + slots[i]
        return total

    total = exchange(devices, me, tile, gathered, tm_copy, ns_sem, nr_sem)
    tile[...] = total
    total = exchange(strips, strip, tile, gathered_z, space_copy, ms_sem, mr_sem)
    summed = jnp.sum(total, axis=1, keepdims=True)
    norms_out[...] = jnp.broadcast_to(jnp.sqrt(summed * (1.0 / cells)), (TILE, 128))

    stores.wait()
    for group in (guess_shift, v0_shift, v1_shift, sol_shift):
        for copy in group:
            @pl.when(jnp.logical_not(last))
            def _():
                copy.wait_send()
    for copy in v1f_shift:
        @pl.when(core == 0)
        def _():
            copy.wait_send()
    for copy in skip_shift:
        @pl.when(sends_skip)
        def _():
            copy.wait_send()
    for _, copy in relays[0::2]:
        copy.wait_send()
    swap.wait_send()
    for i in range(chips):
        owner = core * chips + i
        copy = tm_copy(
            g2h.at[pl.ds(aligned(low - TILE + owner * piece), tall_piece)], c_g2.at[chip, c_rows],
            as_sem.at[i], ar_sem.at[chip], owner,
        )

        @pl.when(owner != me)
        def _():
            copy.wait_send()
    for target, copy in back:
        @pl.when(me != target)
        def _():
            copy.wait_send()


def fast_body(rhs, guess, diffusion):
    devices, strips = lax.axis_size("tm"), lax.axis_size("space")
    rows, width = rhs.shape[1:]
    chips = devices // 2
    cells = rows * strips * width
    height = rows + 2 * EDGE
    c_height = rows // devices + 2 * EDGE

    def plane(*lead):
        return pltpu.VMEM(lead + (height, width), jnp.float32)

    def coarse(count):
        return pltpu.VMEM((count, c_height, width), jnp.float32)

    dma = pltpu.SemaphoreType.DMA
    scratch = [
        plane(2), plane(2), plane(), plane(2), plane(), plane(), plane(), plane(), plane(2),
        plane(), plane(), plane(), plane(), plane(), plane(),
        plane(), plane(), plane(2),
        coarse(chips), coarse(chips), coarse(chips // 2), coarse(chips // 2), coarse(1), coarse(1), coarse(1),
        (coarse(chips // 2), coarse(chips)),
        pltpu.VMEM((TILE, 128), jnp.float32),
        pltpu.VMEM((devices, TILE, 128), jnp.float32),
        pltpu.VMEM((strips, TILE, 128), jnp.float32),
        dma((3,)), dma, dma((5, 2)), dma((5, 2)), dma((5, 4)), dma((5, 4)), dma, dma,
        dma((chips,)), dma((chips,)), dma, dma((2, devices)), dma((2, devices)), dma((2,)),
        dma((chips,)), dma((4,)), dma((4,)),
        dma((devices,)), dma((devices,)), dma((strips,)), dma((strips,)),
    ]
    any_space = pl.BlockSpec(memory_space=pl.ANY)
    result, norms = pl.pallas_call(
        functools.partial(cycle_kernel, strips, devices, cells),
        out_shape=(
            jax.ShapeDtypeStruct(rhs.shape, jnp.float32),
            jax.ShapeDtypeStruct((TILE, 128), jnp.float32),
        ),
        in_specs=[any_space] * 3,
        out_specs=(any_space, pl.BlockSpec(memory_space=pltpu.VMEM)),
        scratch_shapes=scratch,
        compiler_params=pltpu.CompilerParams(
            collective_id=0, has_side_effects=True, vmem_limit_bytes=60 * 2**20
        ),
    )(rhs, guess, diffusion)
    return result, norms[:LEVELS + 1, 0]


def solution(mesh):
    in_specs = (P("tm", "space", None), P("tm", "space", None), P("space", None))
    out_specs = (P("tm", "space", None), P())

    def choose(rhs, guess, diffusion):
        points = rhs.shape[0] * lax.axis_size("tm")
        one_coarsest = points == 2 ** (LEVELS - 1) and rhs.shape[0] == 2
        even = rhs.shape[1] % (TILE * lax.axis_size("tm")) == 0 and rhs.shape[2] % 128 == 0
        if one_coarsest and even:
            return fast_body(rhs, guess, diffusion)
        return body(rhs, guess, diffusion)

    return jax.shard_map(choose, mesh=mesh, in_specs=in_specs, out_specs=out_specs, check_vma=False)
```

```python
import functools

import jax
import jax.numpy as jnp
from jax import lax
from jax.experimental import pallas as pl
from jax.experimental.pallas import tpu as pltpu
from jax.sharding import PartitionSpec as P

LEVELS = 5


damping = 0.8


def with_halo(block, sides, width):
    for axis, dim in sides:
        count = lax.axis_size(axis)
        forward = [(i, i + 1) for i in range(count - 1)]
        backward = [(target, source) for source, target in forward]
        low = lax.ppermute(
            lax.slice_in_dim(block, block.shape[dim] - width, None, axis=dim), axis, forward
        )
        high = lax.ppermute(lax.slice_in_dim(block, 0, width, axis=dim), axis, backward)
        block = jnp.concatenate([low, block, high], axis=dim)
    return block


def shifted(value, axis, steps):
    count = lax.axis_size(axis)
    first, last = (max(0, -steps), min(count, count - steps))
    return lax.ppermute(value, axis, [(source, source + steps) for source in range(first, last)])


def from_partner(value, axis, apart):
    mask = 2**apart
    pairs = [(source, source ^ mask) for source in range(lax.axis_size(axis))]
    return lax.ppermute(value, axis, pairs)


def neighbours(field):
    rows = with_halo(field, (("space", 1),), 1)
    padded = jnp.pad(rows, ((0, 0), (0, 0), (1, 1)))
    total = padded[:, 2:, 1:-1] + padded[:, :-2, 1:-1]
    total = total + padded[:, 1:-1, 2:] + padded[:, 1:-1, :-2]
    return total


def residual(field, source, scaled, diag, stride):
    earlier = shifted(field[-1:], "tm", stride)
    before = jnp.concatenate([earlier, field[:-1]], axis=0)
    image = diag * field - scaled * neighbours(field) - before
    return source - image


def stride_of(level):
    if level == 0:
        return 1
    return 2 ** (level - 1)


def body(rhs, guess, diffusion):
    position = lax.axis_index("tm")
    cells = rhs.shape[1] * lax.axis_size("space") * rhs.shape[2]
    partials = []

    def weight_of(level):
        if level <= 1:
            return jnp.float32(1.0)
        stride = stride_of(level)
        return jnp.where(position % stride == stride - 1, 1.0, 0.0).astype(jnp.float32)

    def record(resid, level):
        local_part = jnp.sum(resid * resid) * weight_of(level)
        partials.append(local_part)

    sources = [rhs]
    fields = []
    field = guess
    for level in range(LEVELS - 1):
        source = sources[level]
        scaled = 2.0**level * diffusion
        diag = 1.0 + 4.0 * scaled
        stride = stride_of(level)
        if level == 0:
            field = field + damping * residual(field, source, scaled, diag, stride) / diag
        else:
            field = damping * source / diag
        resid = residual(field, source, scaled, diag, stride)
        record(resid, level)
        fields.append(field)
        if level == 0:
            coarse = resid[0:1] + resid[1:2]
        else:
            coarse = resid + from_partner(resid, "tm", level - 1)
        sources.append(coarse)
    level = LEVELS - 1
    source = sources[level]
    scaled = 2.0**level * diffusion
    diag = 1.0 + 4.0 * scaled
    stride = stride_of(level)
    field = damping * source / diag
    field = field + damping * residual(field, source, scaled, diag, stride) / diag
    resid = residual(field, source, scaled, diag, stride)
    record(resid, level)
    correction = field
    for level in range(LEVELS - 2, -1, -1):
        scaled = 2.0**level * diffusion
        diag = 1.0 + 4.0 * scaled
        stride = stride_of(level)
        field = fields[level] + correction
        field = field + damping * residual(field, sources[level], scaled, diag, stride) / diag
        correction = field
    scaled = 1.0 * diffusion
    diag = 1.0 + 4.0 * scaled
    resid = residual(correction, rhs, scaled, diag, 1)
    record(resid, 0)
    totals = lax.psum(jnp.stack(partials), ("tm", "space"))
    norms = jnp.sqrt(totals / cells)
    return (correction, norms)


DEVICE = pl.DeviceIdType.MESH
TILE = 8
EDGE = 2 * TILE
BLOCK = 32


def cycle_kernel(
    strips, devices, cells,
    rhs_in, guess_in, diff_in, out, norms_out,
    rhs, guess, diff, v0, g1, v1, r1, v1f, sol, guess_e, v0_e, v1_e, v1_ee, v1f_e, sol_e,
    pair, g2h, v2, c_g2, c_v2, c_g3, c_v3, c_g4, c_v4, c_v4b, finals, weights, tile, gathered, gathered_z,
    load_sem, store_sem, zs_sem, zr_sem, ts_sem, tr_sem, ps_sem, pr_sem, as_sem, ar_sem, al_sem,
    bs_sem, br_sem, bl_sem, rs_sem, es_sem, er_sem, ns_sem, nr_sem, ms_sem, mr_sem,
):
    me = lax.axis_index("tm")
    strip = lax.axis_index("space")
    rows, width = rhs_in.shape[1], rhs_in.shape[2]
    chips = devices // 2
    core = lax.rem(me, 2)
    chip = me // 2
    low, high = EDGE, EDGE + rows
    first, last = me == 0, me == devices - 1
    top, bottom = strip == 0, strip == strips - 1
    piece = rows // devices

    def aligned(value):
        return pl.multiple_of(value, TILE)

    def tm_copy(src, dst, send, recv, target):
        return pltpu.make_async_remote_copy(
            src_ref=src, dst_ref=dst, send_sem=send, recv_sem=recv,
            device_id={"tm": target, "space": strip}, device_id_type=DEVICE,
        )

    def space_copy(src, dst, send, recv, target):
        return pltpu.make_async_remote_copy(
            src_ref=src, dst_ref=dst, send_sem=send, recv_sem=recv,
            device_id={"tm": me, "space": target}, device_id_type=DEVICE,
        )

    later = jnp.minimum(me + 1, devices - 1)
    loads = [
        pltpu.make_async_copy(guess_in, guess.at[:, low:high], load_sem.at[0]),
        pltpu.make_async_copy(diff_in, diff.at[low:high], load_sem.at[1]),
        pltpu.make_async_copy(rhs_in, rhs.at[:, low:high], load_sem.at[2]),
    ]
    for copy in loads:
        copy.start()

    barrier = pltpu.get_barrier_semaphore()
    for i in range(1, devices):
        pl.semaphore_signal(
            barrier, inc=1, device_id={"tm": lax.rem(me + i, devices), "space": strip}, device_id_type=DEVICE
        )
    for i in range(1, strips):
        pl.semaphore_signal(
            barrier, inc=1, device_id={"tm": me, "space": lax.rem(strip + i, strips)}, device_id_type=DEVICE
        )
    pl.semaphore_wait(barrier, devices + strips - 2)

    down = jnp.minimum(strip + 1, strips - 1)
    up = jnp.maximum(strip - 1, 0)

    def halo_pair(index, tail, head, low_dst, high_dst):
        return (
            space_copy(tail, low_dst, zs_sem.at[index, 0], zr_sem.at[index, 0], down),
            space_copy(head, high_dst, zs_sem.at[index, 1], zr_sem.at[index, 1], up),
        )

    before_low, after_high = slice(low - TILE, low), slice(high, high + TILE)
    halos = [
        halo_pair(
            0, guess_in.at[:, rows - TILE:rows], guess_in.at[:, 0:TILE],
            guess.at[:, before_low], guess.at[:, after_high],
        ),
        halo_pair(
            1, diff_in.at[rows - TILE:rows], diff_in.at[0:TILE], diff.at[before_low], diff.at[after_high],
        ),
        halo_pair(
            2, rhs_in.at[:, rows - TILE:rows], rhs_in.at[:, 0:TILE],
            rhs.at[:, before_low], rhs.at[:, after_high],
        ),
    ]

    def start_halo(pair_of):
        @pl.when(jnp.logical_not(bottom))
        def _():
            pair_of[0].start()

        @pl.when(jnp.logical_not(top))
        def _():
            pair_of[1].start()

    def finish_halo(pair_of):
        @pl.when(jnp.logical_not(top))
        def _():
            pair_of[0].wait_recv()
            pair_of[1].wait_send()

        @pl.when(jnp.logical_not(bottom))
        def _():
            pair_of[1].wait_recv()
            pair_of[0].wait_send()

    for pair_of in halos:
        start_halo(pair_of)

    half = rows // 2
    quarter = rows // 4
    whole = [
        (low - TILE, quarter + TILE), (low + quarter, quarter),
        (low + 2 * quarter, quarter), (low + 3 * quarter, quarter + TILE),
    ]
    inner = [(low + quarter * j, quarter) for j in range(4)]
    guess_parts = [(low, half), (low + half, half), (low - TILE, TILE), (high, TILE)]

    def shift(stage, source, target, parts):
        return [
            tm_copy(
                source(start, size), target.at[start:start + size],
                ts_sem.at[stage, j], tr_sem.at[stage, j], later,
            )
            for j, (start, size) in enumerate(parts)
        ]

    def send(copy):
        @pl.when(jnp.logical_not(last))
        def _():
            copy.start()

    def receive(copy):
        @pl.when(jnp.logical_not(first))
        def _():
            copy.wait_recv()

    guess_shift = shift(
        0,
        lambda start, size: (
            guess.at[1, start:start + size] if size == TILE else guess_in.at[1, start - low:start - low + size]
        ),
        guess_e, guess_parts,
    )
    v0_shift = shift(1, lambda start, size: v0.at[1, start:start + size], v0_e, whole)
    v1_shift = shift(2, lambda start, size: v1.at[start:start + size], v1_e, whole)
    v1f_shift = shift(3, lambda start, size: v1f.at[start:start + size], v1f_e, whole)
    sol_shift = shift(4, lambda start, size: sol.at[1, start:start + size], sol_e, inner)
    send(guess_shift[0])
    send(guess_shift[1])

    block = [TILE]

    def at(r):
        return pl.ds(r, block[0])

    def blocks(start, size, step, init=0, ahead=0):
        def loop(begin, count, tall, carry):
            def run(i, carry):
                return step(aligned(begin + i * tall), carry)

            block[0] = tall
            if count == 1:
                carry = step(aligned(begin), carry)
            elif count:
                carry = lax.fori_loop(0, count, run, carry)
            block[0] = TILE
            return carry

        carry = loop(start, ahead // TILE, TILE, init)
        count = (size - ahead) // BLOCK
        carry = loop(start + ahead, count, BLOCK, carry)
        done = ahead + count * BLOCK
        return loop(start + done, (size - done) // TILE, TILE, carry)

    @pl.when(first)
    def _():
        def clear(r, carry):
            zero = jnp.zeros((block[0], width), jnp.float32)
            for ref in (guess_e, v0_e, v1_e, v1_ee, v1f_e, sol_e):
                ref[at(r), :] = zero
            v2[1, at(r), :] = zero
            return carry

        blocks(low - TILE, rows + 2 * TILE, clear, 0, TILE)

    def chunk(j, step, init=0):
        start, size = whole[j]
        return blocks(start, size, step, init, TILE if j == 0 else 0)

    def clear_edge(start):
        for ref in (guess, rhs):
            for p in range(2):
                ref[p, start:start + TILE, :] = jnp.zeros((TILE, width), jnp.float32)
        for p in range(2):
            v2[p, start:start + TILE, :] = jnp.zeros((TILE, width), jnp.float32)
        diff[start:start + TILE, :] = jnp.zeros((TILE, width), jnp.float32)

    @pl.when(top)
    def _():
        clear_edge(low - TILE)

    @pl.when(bottom)
    def _():
        clear_edge(high)

    def stencil(tall):
        size = block[0]
        lane = lax.broadcasted_iota(jnp.int32, (size, width), 1)
        not_left, not_right = lane != 0, lane != width - 1
        mid = tall[TILE:TILE + size]
        total = tall[TILE - 1:TILE + size - 1] + tall[TILE + 1:TILE + size + 1]
        total = total + jnp.where(not_left, pltpu.roll(mid, 1, 1), 0.0)
        total = total + jnp.where(not_right, pltpu.roll(mid, width - 1, 1), 0.0)
        return mid, total

    def tall_at(r):
        return pl.ds(aligned(r - TILE), block[0] + 2 * TILE)

    def coefficients(level, r):
        scaled = 2.0**level * diff[at(r), :]
        diag = 1.0 + 4.0 * scaled
        if level < 2:
            return scaled, diag, weights[level, at(r), :]
        return scaled, diag, damping / diag

    def set_weights(r, carry):
        for level in range(2):
            weights[level, at(r), :] = damping / (1.0 + 4.0 * (2.0**level * diff[at(r), :]))
        return carry

    def squares(value, keep=None):
        square = value * value
        if keep is not None:
            square = jnp.where(keep, square, 0.0)
        total = square[:, 0:128]
        for i in range(1, width // 128):
            total = total + square[:, i * 128:(i + 1) * 128]
        folded = total[0:TILE]
        for i in range(TILE, block[0], TILE):
            folded = folded + total[i:i + TILE]
        return folded

    zero_tile = jnp.zeros((TILE, 128), jnp.float32)
    keep_share = 1.0 - damping

    def sweep_last(r, carry):
        scaled, _, weight = coefficients(0, r)
        mid, total = stencil(guess[1, tall_at(r), :])
        v0[1, at(r), :] = keep_share * mid + weight * (rhs[1, at(r), :] + scaled * total + guess[0, at(r), :])
        return carry

    for copy in loads:
        copy.wait()
    blocks(low, rows, set_weights)
    for j in (1, 2):
        chunk(j, sweep_last)
        send(v0_shift[j])
    finish_halo(halos[0])
    send(guess_shift[2])
    send(guess_shift[3])
    finish_halo(halos[1])
    finish_halo(halos[2])
    blocks(low - TILE, TILE, set_weights)
    blocks(high, TILE, set_weights)
    for j in (0, 3):
        chunk(j, sweep_last)
        send(v0_shift[j])

    def sweep_first(r, carry):
        scaled, _, weight = coefficients(0, r)
        mid, total = stencil(guess[0, tall_at(r), :])
        v0[0, at(r), :] = keep_share * mid + weight * (rhs[0, at(r), :] + scaled * total + guess_e[at(r), :])
        return carry

    for copy in guess_shift:
        receive(copy)
    for j in range(4):
        chunk(j, sweep_first)

    def descend(r, carry):
        keep = jnp.logical_and(r >= low, r < high)
        scaled, diag, _ = coefficients(0, r)
        mid, total = stencil(v0[0, tall_at(r), :])
        one = rhs[0, at(r), :] - diag * mid + scaled * total + v0_e[at(r), :]
        late, total = stencil(v0[1, tall_at(r), :])
        two = rhs[1, at(r), :] - diag * late + scaled * total + mid
        source = one + two
        g1[at(r), :] = source
        _, _, weight = coefficients(1, r)
        v1[at(r), :] = weight * source
        return carry + squares(one, keep) + squares(two, keep)

    total0 = zero_tile
    for j in (1, 2, 0, 3):
        receive(v0_shift[j])
        total0 = chunk(j, descend, total0)
        send(v1_shift[j])

    def residual1(r, carry):
        keep = jnp.logical_and(r >= low, r < high)
        scaled, _, _ = coefficients(1, r)
        _, total = stencil(v1[tall_at(r), :])
        resid = keep_share * g1[at(r), :] + scaled * total + v1_e[at(r), :]
        r1[at(r), :] = resid
        return carry + squares(resid, keep)

    total1 = zero_tile
    for j in (1, 2, 0, 3):
        receive(v1_shift[j])
        total1 = chunk(j, residual1, total1)

    mine = aligned(low - TILE + core * half)
    theirs = aligned(low - TILE + (1 - core) * half)
    span = half + 2 * TILE
    swap = tm_copy(
        r1.at[pl.ds(theirs, span)], pair.at[pl.ds(theirs, span)], ps_sem, pr_sem, me + 1 - 2 * core
    )
    swap.start()
    swap_in = tm_copy(r1.at[pl.ds(mine, span)], pair.at[pl.ds(mine, span)], ps_sem, pr_sem, me + 1 - 2 * core)
    swap_in.wait_recv()

    def join(r, carry):
        g2h[at(r), :] = r1[at(r), :] + pair[at(r), :]
        return carry

    blocks(mine, span, join, 0, TILE)
    tall_piece = piece + 2 * TILE
    c_low, c_high = EDGE, EDGE + piece
    c_rows = slice(c_low - TILE, c_high + TILE)
    for i in range(chips):
        owner = core * chips + i
        src = g2h.at[pl.ds(aligned(low - TILE + owner * piece), tall_piece)]
        copy = tm_copy(src, c_g2.at[chip, c_rows], as_sem.at[i], ar_sem.at[chip], owner)
        local = pltpu.make_async_copy(src, c_g2.at[chip, c_rows], al_sem)

        @pl.when(owner == me)
        def _():
            local.start()
            local.wait()

        @pl.when(owner != me)
        def _():
            copy.start()

    giver = me // chips
    for c in range(chips):
        copy = tm_copy(
            g2h.at[pl.ds(low, tall_piece)], c_g2.at[c, c_rows], as_sem.at[0], ar_sem.at[c],
            lax.rem(me + 1, devices),
        )

        @pl.when(2 * c + giver != me)
        def _():
            copy.wait_recv()

    early_half = ()
    skip_shift = [
        tm_copy(
            v1.at[start:start + size], v1_ee.at[start:start + size], es_sem.at[j], er_sem.at[j],
            jnp.minimum(me + 2, devices - 1),
        )
        for j, (start, size) in enumerate(whole) if j in early_half
    ]
    sends_skip = jnp.logical_and(core == 0, chip < chips - 1)
    has_second = jnp.logical_and(core == 0, jnp.logical_not(first))

    @pl.when(sends_skip)
    def _():
        for copy in skip_shift:
            copy.start()

    offset = me * piece

    def coarse_coefficients(level, r):
        return coefficients(level, aligned(r + offset))


    def coarse(step, init=0):
        return blocks(c_low - TILE, tall_piece, step, init, TILE)

    def first_sweep(level, source, field, count):
        def step(r, carry):
            _, _, weight = coarse_coefficients(level, r)
            for p in range(count):
                field[p, at(r), :] = weight * source[p, at(r), :]
            return carry

        coarse(step)

    def coarse_residual(level, source, field, target, count):
        def step(r, carry):
            keep = jnp.logical_and(r >= c_low, r < c_high)
            scaled, _, _ = coarse_coefficients(level, r)
            earlier, even = None, None
            for p in range(count):
                mid, total = stencil(field[p, tall_at(r), :])
                resid = keep_share * source[p, at(r), :] + scaled * total
                if p:
                    resid = resid + earlier
                earlier = mid
                carry = carry + squares(resid, keep)
                if p % 2 == 0:
                    even = resid
                else:
                    target[p // 2, at(r), :] = even + resid
            return carry

        return coarse(step, zero_tile)

    def ascend(level, source, field, above, target, count):
        def step(r, carry):
            scaled, _, weight = coarse_coefficients(level, r)
            earlier = None
            for p in range(count):
                mid, total = stencil(field[p, tall_at(r), :] + above[p // 2, tall_at(r), :])
                value = source[p, at(r), :] + scaled * total
                if p:
                    value = value + earlier
                earlier = mid
                target[p, at(r), :] = keep_share * mid + weight * value
            return carry

        coarse(step)

    points2, points3 = chips, chips // 2
    first_sweep(2, c_g2, c_v2, points2)
    total2 = coarse_residual(2, c_g2, c_v2, c_g3, points2)
    first_sweep(3, c_g3, c_v3, points3)
    total3 = coarse_residual(3, c_g3, c_v3, c_g4, points3)
    first_sweep(4, c_g4, c_v4, 1)

    def second_sweep(r, carry):
        scaled, _, weight = coarse_coefficients(4, r)
        mid, total = stencil(c_v4[0, tall_at(r), :])
        c_v4b[0, at(r), :] = keep_share * mid + weight * (c_g4[0, at(r), :] + scaled * total)
        return carry

    coarse(second_sweep)

    def residual4(r, carry):
        scaled, diag, _ = coarse_coefficients(4, r)
        mid, total = stencil(c_v4b[0, tall_at(r), :])
        return carry + squares(c_g4[0, at(r), :] - diag * mid + scaled * total)

    total4 = blocks(c_low, piece, residual4, zero_tile)
    c_v3f, c_v2f = finals
    ascend(3, c_g3, c_v3, c_v4b, c_v3f, points3)
    ascend(2, c_g2, c_v2, c_v3f, c_v2f, points2)

    back = []
    place = pl.ds(aligned(low + offset), piece)
    for c in range(chips):
        wants = [(0, 2 * c + core, c)]
        if c > 0:
            wants.append((1, 2 * c, c - 1))
        for kind, target, point in wants:
            src, dst = c_v2f.at[point, c_low:c_high], v2.at[kind, place]
            copy = tm_copy(src, dst, bs_sem.at[kind, c], br_sem.at[kind, me], target)
            local = pltpu.make_async_copy(src, dst, bl_sem.at[kind])
            back.append((target, copy))

            @pl.when(me == target)
            def _():
                local.start()
                local.wait()

            @pl.when(me != target)
            def _():
                copy.start()

    sibling = me + 1 - 2 * core
    relays = []
    for i in range(chips):
        for side in (core, 1 - core):
            k = 2 * i + side
            rows_of = pl.ds(aligned(low + k * piece), piece)
            arrival = tm_copy(v2.at[0, rows_of], v2.at[0, rows_of], rs_sem.at[i], br_sem.at[0, k], sibling)
            relays.append((k, arrival))
    for k, arrival in relays[0::2]:
        @pl.when(k != me)
        def _():
            arrival.wait_recv()

        arrival.start()
    for k, arrival in relays[1::2]:
        arrival.wait_recv()
    for k in range(devices):
        rows_of = slice(low + k * piece, low + (k + 1) * piece)
        arrival = tm_copy(v2.at[1, rows_of], v2.at[1, rows_of], bs_sem.at[1, 0], br_sem.at[1, k], sibling)

        @pl.when(jnp.logical_and(k != me, has_second))
        def _():
            arrival.wait_recv()

    v2_halos = [
        halo_pair(
            3 + kind, v2.at[kind, high - TILE:high], v2.at[kind, low:low + TILE],
            v2.at[kind, before_low], v2.at[kind, after_high],
        )
        for kind in range(2)
    ]
    start_halo(v2_halos[0])

    @pl.when(has_second)
    def _():
        start_halo(v2_halos[1])

    kind = 1 - core

    def ascend1(r, carry):
        scaled, _, weight = coefficients(1, r)
        mid, total = stencil(v1[tall_at(r), :] + v2[0, tall_at(r), :])
        earlier = v1_e[at(r), :] + v2[kind, at(r), :]
        v1f[at(r), :] = keep_share * mid + weight * (g1[at(r), :] + scaled * total + earlier)
        return carry

    for j in (1, 2, 0, 3):
        if j == 0:
            finish_halo(v2_halos[0])

            @pl.when(has_second)
            def _():
                finish_halo(v2_halos[1])

        chunk(j, ascend1)
        if j in early_half:
            @pl.when(core == 0)
            def _():
                v1f_shift[j].start()
        else:
            send(v1f_shift[j])

    def ascend_last(r, carry):
        scaled, _, weight = coefficients(0, r)
        mid, total = stencil(v0[1, tall_at(r), :] + v1f[tall_at(r), :])
        earlier = v0[0, at(r), :] + v1f[at(r), :]
        sol[1, at(r), :] = keep_share * mid + weight * (rhs[1, at(r), :] + scaled * total + earlier)
        return carry

    blocks(low - TILE, TILE, ascend_last, 0)
    for (start, size), copy in zip(inner, sol_shift):
        blocks(start, size, ascend_last, 0)
        send(copy)
    blocks(high, TILE, ascend_last, 0)

    def ascend_first(r, carry):
        scaled, _, weight = coefficients(0, r)
        mid, total = stencil(v0[0, tall_at(r), :] + v1f[tall_at(r), :])
        earlier = v0_e[at(r), :] + v1f_e[at(r), :]
        sol[0, at(r), :] = keep_share * mid + weight * (rhs[0, at(r), :] + scaled * total + earlier)
        return carry

    def ascend_before(r, carry):
        scaled, _, weight = coefficients(1, r)
        early, above = v1_e[at(r), :], v2[1, at(r), :]
        mid, total = stencil(v1_e[tall_at(r), :] + v2[1, tall_at(r), :])
        v1f_e[at(r), :] = keep_share * mid + early + weight * (scaled * total + v1_ee[at(r), :] + above)
        return carry

    for j in range(4):
        if j in early_half:
            @pl.when(core == 1)
            def _():
                v1f_shift[j].wait_recv()

            @pl.when(has_second)
            def _():
                skip_shift[early_half.index(j)].wait_recv()
                chunk(j, ascend_before)
        else:
            receive(v1f_shift[j])

    for j in range(4):
        chunk(j, ascend_first)
    stores = pltpu.make_async_copy(sol.at[:, low:high], out, store_sem)
    stores.start()

    def final_last(r, carry):
        scaled, diag, _ = coefficients(0, r)
        mid, total = stencil(sol[1, tall_at(r), :])
        return carry + squares(rhs[1, at(r), :] - diag * mid + scaled * total + sol[0, at(r), :])

    total5 = blocks(low, rows, final_last, zero_tile)

    def final_first(r, carry):
        scaled, diag, _ = coefficients(0, r)
        mid, total = stencil(sol[0, tall_at(r), :])
        return carry + squares(rhs[0, at(r), :] - diag * mid + scaled * total + sol_e[at(r), :])

    for (start, size), arrived in zip(inner, sol_shift):
        receive(arrived)
        total5 = blocks(start, size, final_first, total5)

    parts = [total0, total1, total2, total3, total4, total5]
    for level, value in enumerate(parts):
        tile[level:level + 1, :] = jnp.sum(value, axis=0, keepdims=True)
    for level in range(len(parts), TILE):
        tile[level:level + 1, :] = jnp.zeros((1, 128), jnp.float32)

    def exchange(count, own, source, slots, copier, send_sems, recv_sems):
        slots[pl.ds(own, 1)] = source[...][None]
        sent = [
            copier(source, slots.at[own], send_sems.at[i], recv_sems.at[own], lax.rem(own + i, count))
            for i in range(1, count)
        ]
        for copy in sent:
            copy.start()
        for i in range(1, count):
            other = lax.rem(own + i, count)
            copier(source, slots.at[other], send_sems.at[i], recv_sems.at[other], other).wait_recv()
        for copy in sent:
            copy.wait_send()
        total = slots[0]
        for i in range(1, count):
            total = total + slots[i]
        return total

    total = exchange(devices, me, tile, gathered, tm_copy, ns_sem, nr_sem)
    tile[...] = total
    total = exchange(strips, strip, tile, gathered_z, space_copy, ms_sem, mr_sem)
    summed = jnp.sum(total, axis=1, keepdims=True)
    norms_out[...] = jnp.broadcast_to(jnp.sqrt(summed * (1.0 / cells)), (TILE, 128))

    stores.wait()
    for group in (guess_shift, v0_shift, v1_shift, sol_shift):
        for copy in group:
            @pl.when(jnp.logical_not(last))
            def _():
                copy.wait_send()
    for j, copy in enumerate(v1f_shift):
        @pl.when((core == 0) if j in early_half else jnp.logical_not(last))
        def _():
            copy.wait_send()
    for copy in skip_shift:
        @pl.when(sends_skip)
        def _():
            copy.wait_send()
    for _, copy in relays[0::2]:
        copy.wait_send()
    swap.wait_send()
    for i in range(chips):
        owner = core * chips + i
        copy = tm_copy(
            g2h.at[pl.ds(aligned(low - TILE + owner * piece), tall_piece)], c_g2.at[chip, c_rows],
            as_sem.at[i], ar_sem.at[chip], owner,
        )

        @pl.when(owner != me)
        def _():
            copy.wait_send()
    for target, copy in back:
        @pl.when(me != target)
        def _():
            copy.wait_send()


def fast_body(rhs, guess, diffusion):
    devices, strips = lax.axis_size("tm"), lax.axis_size("space")
    rows, width = rhs.shape[1:]
    chips = devices // 2
    cells = rows * strips * width
    height = rows + 2 * EDGE
    c_height = rows // devices + 2 * EDGE

    def plane(*lead):
        return pltpu.VMEM(lead + (height, width), jnp.float32)

    def coarse(count):
        return pltpu.VMEM((count, c_height, width), jnp.float32)

    dma = pltpu.SemaphoreType.DMA
    scratch = [
        plane(2), plane(2), plane(), plane(2), plane(), plane(), plane(), plane(), plane(2),
        plane(), plane(), plane(), plane(), plane(), plane(),
        plane(), plane(), plane(2),
        coarse(chips), coarse(chips), coarse(chips // 2), coarse(chips // 2), coarse(1), coarse(1), coarse(1),
        (coarse(chips // 2), coarse(chips)),
        plane(2),
        pltpu.VMEM((TILE, 128), jnp.float32),
        pltpu.VMEM((devices, TILE, 128), jnp.float32),
        pltpu.VMEM((strips, TILE, 128), jnp.float32),
        dma((3,)), dma, dma((5, 2)), dma((5, 2)), dma((5, 4)), dma((5, 4)), dma, dma,
        dma((chips,)), dma((chips,)), dma, dma((2, devices)), dma((2, devices)), dma((2,)),
        dma((chips,)), dma((4,)), dma((4,)),
        dma((devices,)), dma((devices,)), dma((strips,)), dma((strips,)),
    ]
    any_space = pl.BlockSpec(memory_space=pl.ANY)
    result, norms = pl.pallas_call(
        functools.partial(cycle_kernel, strips, devices, cells),
        out_shape=(
            jax.ShapeDtypeStruct(rhs.shape, jnp.float32),
            jax.ShapeDtypeStruct((TILE, 128), jnp.float32),
        ),
        in_specs=[any_space] * 3,
        out_specs=(any_space, pl.BlockSpec(memory_space=pltpu.VMEM)),
        scratch_shapes=scratch,
        compiler_params=pltpu.CompilerParams(
            collective_id=0, has_side_effects=True, vmem_limit_bytes=60 * 2**20
        ),
    )(rhs, guess, diffusion)
    return result, norms[:LEVELS + 1, 0]


def solution(mesh):
    in_specs = (P("tm", "space", None), P("tm", "space", None), P("space", None))
    out_specs = (P("tm", "space", None), P())

    def choose(rhs, guess, diffusion):
        points = rhs.shape[0] * lax.axis_size("tm")
        one_coarsest = points == 2 ** (LEVELS - 1) and rhs.shape[0] == 2
        even = rhs.shape[1] % (TILE * lax.axis_size("tm")) == 0 and rhs.shape[2] % 128 == 0
        if one_coarsest and even:
            return fast_body(rhs, guess, diffusion)
        return body(rhs, guess, diffusion)

    return jax.shard_map(choose, mesh=mesh, in_specs=in_specs, out_specs=out_specs, check_vma=False)
```

```python
import functools

import jax
import jax.numpy as jnp
from jax import lax
from jax.experimental import pallas as pl
from jax.experimental.pallas import tpu as pltpu
from jax.sharding import PartitionSpec as P

LEVELS = 5


damping = 0.8


def with_halo(block, sides, width):
    for axis, dim in sides:
        count = lax.axis_size(axis)
        forward = [(i, i + 1) for i in range(count - 1)]
        backward = [(target, source) for source, target in forward]
        low = lax.ppermute(
            lax.slice_in_dim(block, block.shape[dim] - width, None, axis=dim), axis, forward
        )
        high = lax.ppermute(lax.slice_in_dim(block, 0, width, axis=dim), axis, backward)
        block = jnp.concatenate([low, block, high], axis=dim)
    return block


def shifted(value, axis, steps):
    count = lax.axis_size(axis)
    first, last = (max(0, -steps), min(count, count - steps))
    return lax.ppermute(value, axis, [(source, source + steps) for source in range(first, last)])


def from_partner(value, axis, apart):
    mask = 2**apart
    pairs = [(source, source ^ mask) for source in range(lax.axis_size(axis))]
    return lax.ppermute(value, axis, pairs)


def neighbours(field):
    rows = with_halo(field, (("space", 1),), 1)
    padded = jnp.pad(rows, ((0, 0), (0, 0), (1, 1)))
    total = padded[:, 2:, 1:-1] + padded[:, :-2, 1:-1]
    total = total + padded[:, 1:-1, 2:] + padded[:, 1:-1, :-2]
    return total


def residual(field, source, scaled, diag, stride):
    earlier = shifted(field[-1:], "tm", stride)
    before = jnp.concatenate([earlier, field[:-1]], axis=0)
    image = diag * field - scaled * neighbours(field) - before
    return source - image


def stride_of(level):
    if level == 0:
        return 1
    return 2 ** (level - 1)


def body(rhs, guess, diffusion):
    position = lax.axis_index("tm")
    cells = rhs.shape[1] * lax.axis_size("space") * rhs.shape[2]
    partials = []

    def weight_of(level):
        if level <= 1:
            return jnp.float32(1.0)
        stride = stride_of(level)
        return jnp.where(position % stride == stride - 1, 1.0, 0.0).astype(jnp.float32)

    def record(resid, level):
        local_part = jnp.sum(resid * resid) * weight_of(level)
        partials.append(local_part)

    sources = [rhs]
    fields = []
    field = guess
    for level in range(LEVELS - 1):
        source = sources[level]
        scaled = 2.0**level * diffusion
        diag = 1.0 + 4.0 * scaled
        stride = stride_of(level)
        if level == 0:
            field = field + damping * residual(field, source, scaled, diag, stride) / diag
        else:
            field = damping * source / diag
        resid = residual(field, source, scaled, diag, stride)
        record(resid, level)
        fields.append(field)
        if level == 0:
            coarse = resid[0:1] + resid[1:2]
        else:
            coarse = resid + from_partner(resid, "tm", level - 1)
        sources.append(coarse)
    level = LEVELS - 1
    source = sources[level]
    scaled = 2.0**level * diffusion
    diag = 1.0 + 4.0 * scaled
    stride = stride_of(level)
    field = damping * source / diag
    field = field + damping * residual(field, source, scaled, diag, stride) / diag
    resid = residual(field, source, scaled, diag, stride)
    record(resid, level)
    correction = field
    for level in range(LEVELS - 2, -1, -1):
        scaled = 2.0**level * diffusion
        diag = 1.0 + 4.0 * scaled
        stride = stride_of(level)
        field = fields[level] + correction
        field = field + damping * residual(field, sources[level], scaled, diag, stride) / diag
        correction = field
    scaled = 1.0 * diffusion
    diag = 1.0 + 4.0 * scaled
    resid = residual(correction, rhs, scaled, diag, 1)
    record(resid, 0)
    totals = lax.psum(jnp.stack(partials), ("tm", "space"))
    norms = jnp.sqrt(totals / cells)
    return (correction, norms)


DEVICE = pl.DeviceIdType.MESH
TILE = 8
EDGE = 2 * TILE
BLOCK = 32


def cycle_kernel(
    strips, devices, cells,
    rhs_in, guess_in, diff_in, out, norms_out,
    rhs, guess, diff, v0, g1, v1, r1, v1f, sol, guess_e, v0_e, v1_e, v1f_e, sol_e,
    pair, g2h, v2, c_g2, c_v2, c_g3, c_v3, c_g4, c_v4, c_v4b, finals, weights, tile, gathered, gathered_z,
    load_sem, store_sem, zs_sem, zr_sem, ts_sem, tr_sem, ps_sem, pr_sem, as_sem, ar_sem, al_sem,
    bs_sem, br_sem, bl_sem, rs_sem, credit, ns_sem, nr_sem, ms_sem, mr_sem,
):
    me = lax.axis_index("tm")
    strip = lax.axis_index("space")
    rows, width = rhs_in.shape[1], rhs_in.shape[2]
    chips = devices // 2
    core = lax.rem(me, 2)
    chip = me // 2
    low, high = EDGE, EDGE + rows
    first, last = me == 0, me == devices - 1
    top, bottom = strip == 0, strip == strips - 1
    piece = rows // devices

    def aligned(value):
        return pl.multiple_of(value, TILE)

    def tm_copy(src, dst, send, recv, target):
        return pltpu.make_async_remote_copy(
            src_ref=src, dst_ref=dst, send_sem=send, recv_sem=recv,
            device_id={"tm": target, "space": strip}, device_id_type=DEVICE,
        )

    def space_copy(src, dst, send, recv, target):
        return pltpu.make_async_remote_copy(
            src_ref=src, dst_ref=dst, send_sem=send, recv_sem=recv,
            device_id={"tm": me, "space": target}, device_id_type=DEVICE,
        )

    later = jnp.minimum(me + 1, devices - 1)
    loads = [
        pltpu.make_async_copy(guess_in, guess.at[:, low:high], load_sem.at[0]),
        pltpu.make_async_copy(diff_in, diff.at[low:high], load_sem.at[1]),
        pltpu.make_async_copy(rhs_in, rhs.at[:, low:high], load_sem.at[2]),
    ]
    for copy in loads:
        copy.start()

    barrier = pltpu.get_barrier_semaphore()
    for i in range(1, devices):
        pl.semaphore_signal(
            barrier, inc=1, device_id={"tm": lax.rem(me + i, devices), "space": strip}, device_id_type=DEVICE
        )
    for i in range(1, strips):
        pl.semaphore_signal(
            barrier, inc=1, device_id={"tm": me, "space": lax.rem(strip + i, strips)}, device_id_type=DEVICE
        )
    pl.semaphore_wait(barrier, devices + strips - 2)

    down = jnp.minimum(strip + 1, strips - 1)
    up = jnp.maximum(strip - 1, 0)

    def halo_pair(index, tail, head, low_dst, high_dst):
        return (
            space_copy(tail, low_dst, zs_sem.at[index, 0], zr_sem.at[index, 0], down),
            space_copy(head, high_dst, zs_sem.at[index, 1], zr_sem.at[index, 1], up),
        )

    before_low, after_high = slice(low - TILE, low), slice(high, high + TILE)
    halos = [
        halo_pair(
            0, guess_in.at[:, rows - TILE:rows], guess_in.at[:, 0:TILE],
            guess.at[:, before_low], guess.at[:, after_high],
        ),
        halo_pair(
            1, diff_in.at[rows - TILE:rows], diff_in.at[0:TILE], diff.at[before_low], diff.at[after_high],
        ),
        halo_pair(
            2, rhs_in.at[:, rows - TILE:rows], rhs_in.at[:, 0:TILE],
            rhs.at[:, before_low], rhs.at[:, after_high],
        ),
    ]

    def start_halo(pair_of):
        @pl.when(jnp.logical_not(bottom))
        def _():
            pair_of[0].start()

        @pl.when(jnp.logical_not(top))
        def _():
            pair_of[1].start()

    def finish_halo(pair_of):
        @pl.when(jnp.logical_not(top))
        def _():
            pair_of[0].wait_recv()
            pair_of[1].wait_send()

        @pl.when(jnp.logical_not(bottom))
        def _():
            pair_of[1].wait_recv()
            pair_of[0].wait_send()

    for pair_of in halos:
        start_halo(pair_of)

    half = rows // 2
    quarter = rows // 4
    whole = [
        (low - TILE, quarter + TILE), (low + quarter, quarter),
        (low + 2 * quarter, quarter), (low + 3 * quarter, quarter + TILE),
    ]
    inner = [(low + quarter * j, quarter) for j in range(4)]
    guess_parts = [(low, half), (low + half, half), (low - TILE, TILE), (high, TILE)]

    def shift(stage, source, target, parts):
        return [
            tm_copy(
                source(start, size), target.at[start:start + size],
                ts_sem.at[stage, j], tr_sem.at[stage, j], later,
            )
            for j, (start, size) in enumerate(parts)
        ]

    def send(copy):
        @pl.when(jnp.logical_not(last))
        def _():
            copy.start()

    def receive(copy):
        @pl.when(jnp.logical_not(first))
        def _():
            copy.wait_recv()

    guess_shift = shift(
        0,
        lambda start, size: (
            guess.at[1, start:start + size] if size == TILE else guess_in.at[1, start - low:start - low + size]
        ),
        guess_e, guess_parts,
    )
    v0_shift = shift(1, lambda start, size: v0.at[1, start:start + size], v0_e, whole)
    v1_shift = shift(2, lambda start, size: v1.at[start:start + size], v1_e, whole)
    v1f_shift = shift(3, lambda start, size: v1f.at[start:start + size], v1f_e, whole)
    sol_shift = shift(4, lambda start, size: sol.at[1, start:start + size], sol_e, inner)
    send(guess_shift[0])
    send(guess_shift[1])

    block = [TILE]

    def at(r):
        return pl.ds(r, block[0])

    def blocks(start, size, step, init=0, ahead=0):
        def loop(begin, count, tall, carry):
            def run(i, carry):
                return step(aligned(begin + i * tall), carry)

            block[0] = tall
            if count == 1:
                carry = step(aligned(begin), carry)
            elif count:
                carry = lax.fori_loop(0, count, run, carry)
            block[0] = TILE
            return carry

        carry = loop(start, ahead // TILE, TILE, init)
        count = (size - ahead) // BLOCK
        carry = loop(start + ahead, count, BLOCK, carry)
        done = ahead + count * BLOCK
        return loop(start + done, (size - done) // TILE, TILE, carry)

    @pl.when(first)
    def _():
        def clear(r, carry):
            zero = jnp.zeros((block[0], width), jnp.float32)
            for ref in (guess_e, v0_e, v1_e, v1f_e, sol_e):
                ref[at(r), :] = zero
            v2[1, at(r), :] = zero
            return carry

        blocks(low - TILE, rows + 2 * TILE, clear, 0, TILE)

    def chunk(j, step, init=0):
        start, size = whole[j]
        return blocks(start, size, step, init, TILE if j == 0 else 0)

    def clear_edge(start):
        for ref in (guess, rhs):
            for p in range(2):
                ref[p, start:start + TILE, :] = jnp.zeros((TILE, width), jnp.float32)
        for p in range(2):
            v2[p, start:start + TILE, :] = jnp.zeros((TILE, width), jnp.float32)
        diff[start:start + TILE, :] = jnp.zeros((TILE, width), jnp.float32)

    @pl.when(top)
    def _():
        clear_edge(low - TILE)

    @pl.when(bottom)
    def _():
        clear_edge(high)

    def stencil(tall):
        size = block[0]
        lane = lax.broadcasted_iota(jnp.int32, (size, width), 1)
        not_left, not_right = lane != 0, lane != width - 1
        mid = tall[TILE:TILE + size]
        total = tall[TILE - 1:TILE + size - 1] + tall[TILE + 1:TILE + size + 1]
        total = total + jnp.where(not_left, pltpu.roll(mid, 1, 1), 0.0)
        total = total + jnp.where(not_right, pltpu.roll(mid, width - 1, 1), 0.0)
        return mid, total

    def tall_at(r):
        return pl.ds(aligned(r - TILE), block[0] + 2 * TILE)

    def coefficients(level, r):
        scaled = 2.0**level * diff[at(r), :]
        diag = 1.0 + 4.0 * scaled
        if level < 2:
            return scaled, diag, weights[level, at(r), :]
        return scaled, diag, damping / diag

    def set_weights(r, carry):
        for level in range(2):
            weights[level, at(r), :] = damping / (1.0 + 4.0 * (2.0**level * diff[at(r), :]))
        return carry

    def squares(value, keep=None):
        square = value * value
        if keep is not None:
            square = jnp.where(keep, square, 0.0)
        total = square[:, 0:128]
        for i in range(1, width // 128):
            total = total + square[:, i * 128:(i + 1) * 128]
        folded = total[0:TILE]
        for i in range(TILE, block[0], TILE):
            folded = folded + total[i:i + TILE]
        return folded

    zero_tile = jnp.zeros((TILE, 128), jnp.float32)
    keep_share = 1.0 - damping

    def sweep_last(r, carry):
        scaled, _, weight = coefficients(0, r)
        mid, total = stencil(guess[1, tall_at(r), :])
        v0[1, at(r), :] = keep_share * mid + weight * (rhs[1, at(r), :] + scaled * total + guess[0, at(r), :])
        return carry

    for copy in loads:
        copy.wait()
    blocks(low, rows, set_weights)
    for j in (1, 2):
        chunk(j, sweep_last)
        send(v0_shift[j])
    finish_halo(halos[0])
    send(guess_shift[2])
    send(guess_shift[3])
    finish_halo(halos[1])
    finish_halo(halos[2])
    blocks(low - TILE, TILE, set_weights)
    blocks(high, TILE, set_weights)
    for j in (0, 3):
        chunk(j, sweep_last)
        send(v0_shift[j])

    def sweep_first(r, carry):
        scaled, _, weight = coefficients(0, r)
        mid, total = stencil(guess[0, tall_at(r), :])
        v0[0, at(r), :] = keep_share * mid + weight * (rhs[0, at(r), :] + scaled * total + guess_e[at(r), :])
        return carry

    for copy in guess_shift:
        receive(copy)
    for j in range(4):
        chunk(j, sweep_first)

    def descend(r, carry):
        keep = jnp.logical_and(r >= low, r < high)
        scaled, diag, _ = coefficients(0, r)
        mid, total = stencil(v0[0, tall_at(r), :])
        one = rhs[0, at(r), :] - diag * mid + scaled * total + v0_e[at(r), :]
        late, total = stencil(v0[1, tall_at(r), :])
        two = rhs[1, at(r), :] - diag * late + scaled * total + mid
        source = one + two
        g1[at(r), :] = source
        _, _, weight = coefficients(1, r)
        v1[at(r), :] = weight * source
        return carry + squares(one, keep) + squares(two, keep)

    total0 = zero_tile
    for j in range(4):
        receive(v0_shift[j])
        total0 = chunk(j, descend, total0)
        send(v1_shift[j])

    def residual1(r, carry):
        keep = jnp.logical_and(r >= low, r < high)
        scaled, _, _ = coefficients(1, r)
        _, total = stencil(v1[tall_at(r), :])
        resid = keep_share * g1[at(r), :] + scaled * total + v1_e[at(r), :]
        r1[at(r), :] = resid
        return carry + squares(resid, keep)

    total1 = zero_tile
    tall_piece = piece + 2 * TILE
    c_low, c_high = EDGE, EDGE + piece
    c_rows = slice(c_low - TILE, c_high + TILE)
    sibling = me + 1 - 2 * core

    def swap_of(k):
        start = low - TILE + k * piece
        return tm_copy(
            r1.at[start:start + tall_piece], pair.at[k // 2], ps_sem.at[k // 2], pr_sem.at[k // 2], sibling
        )

    def hand_over(k):
        return tm_copy(g2h.at[k // 2], c_g2.at[chip, c_rows], as_sem.at[k // 2], ar_sem.at[chip], k)

    def join_piece(k):
        start = low - TILE + k * piece

        def join(r, carry):
            g2h[k // 2, at(r), :] = r1[at(aligned(r + start)), :] + pair[k // 2, at(r), :]
            return carry

        swap_of(k).wait_recv()
        blocks(0, tall_piece, join, 0, TILE)
        local = pltpu.make_async_copy(g2h.at[k // 2], c_g2.at[chip, c_rows], al_sem)

        @pl.when(me == k)
        def _():
            local.start()
            local.wait()

        @pl.when(me != k)
        def _():
            hand_over(k).start()

    done = 0
    for j in range(4):
        receive(v1_shift[j])
        total1 = chunk(j, residual1, total1)
        ready = (sum(whole[j]) - tall_piece - low + TILE) // piece + 1
        for k in range(done, ready):
            @pl.when(core != k % 2)
            def _():
                swap_of(k).start()
        for k in range(done, ready):
            @pl.when(core == k % 2)
            def _():
                join_piece(k)
        done = ready
    for c in range(chips):
        copy = tm_copy(g2h.at[0], c_g2.at[c, c_rows], as_sem.at[0], ar_sem.at[c], sibling)

        @pl.when(c != chip)
        def _():
            copy.wait_recv()

    has_second = jnp.logical_and(core == 0, jnp.logical_not(first))

    offset = me * piece

    def coarse_coefficients(level, r):
        return coefficients(level, aligned(r + offset))


    def coarse(step, init=0):
        return blocks(c_low - TILE, tall_piece, step, init, TILE)

    def first_sweep(level, source, field, count):
        def step(r, carry):
            _, _, weight = coarse_coefficients(level, r)
            for p in range(count):
                field[p, at(r), :] = weight * source[p, at(r), :]
            return carry

        coarse(step)

    def coarse_residual(level, source, field, target, count):
        def step(r, carry):
            keep = jnp.logical_and(r >= c_low, r < c_high)
            scaled, _, _ = coarse_coefficients(level, r)
            earlier, even = None, None
            for p in range(count):
                mid, total = stencil(field[p, tall_at(r), :])
                resid = keep_share * source[p, at(r), :] + scaled * total
                if p:
                    resid = resid + earlier
                earlier = mid
                carry = carry + squares(resid, keep)
                if p % 2 == 0:
                    even = resid
                else:
                    target[p // 2, at(r), :] = even + resid
            return carry

        return coarse(step, zero_tile)

    def ascend(level, source, field, above, target, count):
        def step(r, carry):
            scaled, _, weight = coarse_coefficients(level, r)
            earlier = None
            for p in range(count):
                mid, total = stencil(field[p, tall_at(r), :] + above[p // 2, tall_at(r), :])
                value = source[p, at(r), :] + scaled * total
                if p:
                    value = value + earlier
                earlier = mid
                target[p, at(r), :] = keep_share * mid + weight * value
            return carry

        coarse(step)

    points2, points3 = chips, chips // 2
    first_sweep(2, c_g2, c_v2, points2)
    total2 = coarse_residual(2, c_g2, c_v2, c_g3, points2)
    first_sweep(3, c_g3, c_v3, points3)
    total3 = coarse_residual(3, c_g3, c_v3, c_g4, points3)
    first_sweep(4, c_g4, c_v4, 1)

    def second_sweep(r, carry):
        scaled, _, weight = coarse_coefficients(4, r)
        mid, total = stencil(c_v4[0, tall_at(r), :])
        c_v4b[0, at(r), :] = keep_share * mid + weight * (c_g4[0, at(r), :] + scaled * total)
        return carry

    coarse(second_sweep)

    def residual4(r, carry):
        scaled, diag, _ = coarse_coefficients(4, r)
        mid, total = stencil(c_v4b[0, tall_at(r), :])
        return carry + squares(c_g4[0, at(r), :] - diag * mid + scaled * total)

    total4 = blocks(c_low, piece, residual4, zero_tile)
    c_v3f, c_v2f = finals
    ascend(3, c_g3, c_v3, c_v4b, c_v3f, points3)
    ascend(2, c_g2, c_v2, c_v3f, c_v2f, points2)

    back = []
    place = pl.ds(aligned(low + offset), piece)
    for c in range(chips):
        wants = [(0, 2 * c + core, c)]
        if c > 0:
            wants.append((1, 2 * c, c - 1))
        for kind, target, point in wants:
            src, dst = c_v2f.at[point, c_low:c_high], v2.at[kind, place]
            copy = tm_copy(src, dst, bs_sem.at[kind, c], br_sem.at[kind, me], target)
            local = pltpu.make_async_copy(src, dst, bl_sem.at[kind])
            back.append((target, copy))

            @pl.when(me == target)
            def _():
                local.start()
                local.wait()

            @pl.when(me != target)
            def _():
                copy.start()

    relays = []
    for i in range(chips):
        for side in (core, 1 - core):
            k = 2 * i + side
            rows_of = pl.ds(aligned(low + k * piece), piece)
            arrival = tm_copy(v2.at[0, rows_of], v2.at[0, rows_of], rs_sem.at[i], br_sem.at[0, k], sibling)
            relays.append((k, arrival))
    for k, arrival in relays[0::2]:
        @pl.when(k != me)
        def _():
            arrival.wait_recv()

        arrival.start()
    for k, arrival in relays[1::2]:
        arrival.wait_recv()
    for k in range(devices):
        rows_of = slice(low + k * piece, low + (k + 1) * piece)
        arrival = tm_copy(v2.at[1, rows_of], v2.at[1, rows_of], bs_sem.at[1, 0], br_sem.at[1, k], sibling)

        @pl.when(jnp.logical_and(k != me, has_second))
        def _():
            arrival.wait_recv()

    v2_halos = [
        halo_pair(
            3 + kind, v2.at[kind, high - TILE:high], v2.at[kind, low:low + TILE],
            v2.at[kind, before_low], v2.at[kind, after_high],
        )
        for kind in range(2)
    ]
    start_halo(v2_halos[0])

    @pl.when(has_second)
    def _():
        start_halo(v2_halos[1])

    sends_on = jnp.logical_and(core == 1, jnp.logical_not(last))

    @pl.when(has_second)
    def _():
        pl.semaphore_signal(credit, inc=1, device_id={"tm": me - 1, "space": strip}, device_id_type=DEVICE)

    kind = 1 - core

    def ascend1(r, carry):
        scaled, _, weight = coefficients(1, r)
        mid, total = stencil(v1[tall_at(r), :] + v2[0, tall_at(r), :])
        earlier = v1_e[at(r), :] + v2[kind, at(r), :]
        v1f[at(r), :] = keep_share * mid + weight * (g1[at(r), :] + scaled * total + earlier)
        return carry

    for j in (1, 2, 0, 3):
        if j == 0:
            finish_halo(v2_halos[0])

            @pl.when(has_second)
            def _():
                finish_halo(v2_halos[1])

        chunk(j, ascend1)
        if j == 1:
            @pl.when(sends_on)
            def _():
                pl.semaphore_wait(credit, 1)
        send(v1f_shift[j])

    def ascend_last(r, carry):
        scaled, _, weight = coefficients(0, r)
        mid, total = stencil(v0[1, tall_at(r), :] + v1f[tall_at(r), :])
        earlier = v0[0, at(r), :] + v1f[at(r), :]
        sol[1, at(r), :] = keep_share * mid + weight * (rhs[1, at(r), :] + scaled * total + earlier)
        return carry

    blocks(low - TILE, TILE, ascend_last, 0)
    for start, size in inner:
        blocks(start, size, ascend_last, 0)
    blocks(high, TILE, ascend_last, 0)

    def ascend_first(r, carry):
        scaled, _, weight = coefficients(0, r)
        mid, total = stencil(v0[0, tall_at(r), :] + v1f[tall_at(r), :])
        earlier = v0_e[at(r), :] + v1f_e[at(r), :]
        sol[0, at(r), :] = keep_share * mid + weight * (rhs[0, at(r), :] + scaled * total + earlier)
        return carry

    for j in range(4):
        receive(v1f_shift[j])

        @pl.when(jnp.logical_not(last))
        def _():
            v1f_shift[j].wait_send()
            sol_shift[j].start()

        chunk(j, ascend_first)
    stores = pltpu.make_async_copy(sol.at[:, low:high], out, store_sem)
    stores.start()

    def final_last(r, carry):
        scaled, diag, _ = coefficients(0, r)
        mid, total = stencil(sol[1, tall_at(r), :])
        return carry + squares(rhs[1, at(r), :] - diag * mid + scaled * total + sol[0, at(r), :])

    total5 = blocks(low, rows, final_last, zero_tile)

    def final_first(r, carry):
        scaled, diag, _ = coefficients(0, r)
        mid, total = stencil(sol[0, tall_at(r), :])
        return carry + squares(rhs[0, at(r), :] - diag * mid + scaled * total + sol_e[at(r), :])

    for (start, size), arrived in zip(inner, sol_shift):
        receive(arrived)
        total5 = blocks(start, size, final_first, total5)

    parts = [total0, total1, total2, total3, total4, total5]
    for level, value in enumerate(parts):
        tile[level:level + 1, :] = jnp.sum(value, axis=0, keepdims=True)
    for level in range(len(parts), TILE):
        tile[level:level + 1, :] = jnp.zeros((1, 128), jnp.float32)

    def exchange(count, own, source, slots, copier, send_sems, recv_sems):
        slots[pl.ds(own, 1)] = source[...][None]
        sent = [
            copier(source, slots.at[own], send_sems.at[i], recv_sems.at[own], lax.rem(own + i, count))
            for i in range(1, count)
        ]
        for copy in sent:
            copy.start()
        for i in range(1, count):
            other = lax.rem(own + i, count)
            copier(source, slots.at[other], send_sems.at[i], recv_sems.at[other], other).wait_recv()
        for copy in sent:
            copy.wait_send()
        total = slots[0]
        for i in range(1, count):
            total = total + slots[i]
        return total

    total = exchange(devices, me, tile, gathered, tm_copy, ns_sem, nr_sem)
    tile[...] = total
    total = exchange(strips, strip, tile, gathered_z, space_copy, ms_sem, mr_sem)
    summed = jnp.sum(total, axis=1, keepdims=True)
    norms_out[...] = jnp.broadcast_to(jnp.sqrt(summed * (1.0 / cells)), (TILE, 128))

    stores.wait()
    for group in (guess_shift, v0_shift, v1_shift, sol_shift):
        for copy in group:
            @pl.when(jnp.logical_not(last))
            def _():
                copy.wait_send()
    for _, copy in relays[0::2]:
        copy.wait_send()
    for k in range(devices):
        @pl.when(core != k % 2)
        def _():
            swap_of(k).wait_send()

        @pl.when(jnp.logical_and(core == k % 2, me != k))
        def _():
            hand_over(k).wait_send()
    for target, copy in back:
        @pl.when(me != target)
        def _():
            copy.wait_send()


def fast_body(rhs, guess, diffusion):
    devices, strips = lax.axis_size("tm"), lax.axis_size("space")
    rows, width = rhs.shape[1:]
    chips = devices // 2
    cells = rows * strips * width
    height = rows + 2 * EDGE
    c_height = rows // devices + 2 * EDGE

    def plane(*lead):
        return pltpu.VMEM(lead + (height, width), jnp.float32)

    def coarse(count):
        return pltpu.VMEM((count, c_height, width), jnp.float32)

    shared = pltpu.VMEM((chips, rows // devices + EDGE, width), jnp.float32)
    dma = pltpu.SemaphoreType.DMA
    scratch = [
        plane(2), plane(2), plane(), plane(2), plane(), plane(), plane(), plane(), plane(2),
        plane(), plane(), plane(), plane(), plane(),
        shared, shared, plane(2),
        coarse(chips), coarse(chips), coarse(chips // 2), coarse(chips // 2), coarse(1), coarse(1), coarse(1),
        (coarse(chips // 2), coarse(chips)),
        plane(2),
        pltpu.VMEM((TILE, 128), jnp.float32),
        pltpu.VMEM((devices, TILE, 128), jnp.float32),
        pltpu.VMEM((strips, TILE, 128), jnp.float32),
        dma((3,)), dma, dma((5, 2)), dma((5, 2)), dma((5, 4)), dma((5, 4)), dma((chips,)), dma((chips,)),
        dma((chips,)), dma((chips,)), dma, dma((2, devices)), dma((2, devices)), dma((2,)),
        dma((chips,)), pltpu.SemaphoreType.REGULAR,
        dma((devices,)), dma((devices,)), dma((strips,)), dma((strips,)),
    ]
    any_space = pl.BlockSpec(memory_space=pl.ANY)
    result, norms = pl.pallas_call(
        functools.partial(cycle_kernel, strips, devices, cells),
        out_shape=(
            jax.ShapeDtypeStruct(rhs.shape, jnp.float32),
            jax.ShapeDtypeStruct((TILE, 128), jnp.float32),
        ),
        in_specs=[any_space] * 3,
        out_specs=(any_space, pl.BlockSpec(memory_space=pltpu.VMEM)),
        scratch_shapes=scratch,
        compiler_params=pltpu.CompilerParams(
            collective_id=0, has_side_effects=True, vmem_limit_bytes=60 * 2**20
        ),
    )(rhs, guess, diffusion)
    return result, norms[:LEVELS + 1, 0]


def solution(mesh):
    in_specs = (P("tm", "space", None), P("tm", "space", None), P("space", None))
    out_specs = (P("tm", "space", None), P())

    def choose(rhs, guess, diffusion):
        points = rhs.shape[0] * lax.axis_size("tm")
        one_coarsest = points == 2 ** (LEVELS - 1) and rhs.shape[0] == 2
        even = rhs.shape[1] % (TILE * lax.axis_size("tm")) == 0 and rhs.shape[2] % 128 == 0
        if one_coarsest and even:
            return fast_body(rhs, guess, diffusion)
        return body(rhs, guess, diffusion)

    return jax.shard_map(choose, mesh=mesh, in_specs=in_specs, out_specs=out_specs, check_vma=False)
```

```python
import functools

import jax
import jax.numpy as jnp
from jax import lax
from jax.experimental import pallas as pl
from jax.experimental.pallas import tpu as pltpu
from jax.sharding import PartitionSpec as P

LEVELS = 5


damping = 0.8


def with_halo(block, sides, width):
    for axis, dim in sides:
        count = lax.axis_size(axis)
        forward = [(i, i + 1) for i in range(count - 1)]
        backward = [(target, source) for source, target in forward]
        low = lax.ppermute(
            lax.slice_in_dim(block, block.shape[dim] - width, None, axis=dim), axis, forward
        )
        high = lax.ppermute(lax.slice_in_dim(block, 0, width, axis=dim), axis, backward)
        block = jnp.concatenate([low, block, high], axis=dim)
    return block


def shifted(value, axis, steps):
    count = lax.axis_size(axis)
    first, last = (max(0, -steps), min(count, count - steps))
    return lax.ppermute(value, axis, [(source, source + steps) for source in range(first, last)])


def from_partner(value, axis, apart):
    mask = 2**apart
    pairs = [(source, source ^ mask) for source in range(lax.axis_size(axis))]
    return lax.ppermute(value, axis, pairs)


def neighbours(field):
    rows = with_halo(field, (("space", 1),), 1)
    padded = jnp.pad(rows, ((0, 0), (0, 0), (1, 1)))
    total = padded[:, 2:, 1:-1] + padded[:, :-2, 1:-1]
    total = total + padded[:, 1:-1, 2:] + padded[:, 1:-1, :-2]
    return total


def residual(field, source, scaled, diag, stride):
    earlier = shifted(field[-1:], "tm", stride)
    before = jnp.concatenate([earlier, field[:-1]], axis=0)
    image = diag * field - scaled * neighbours(field) - before
    return source - image


def stride_of(level):
    if level == 0:
        return 1
    return 2 ** (level - 1)


def body(rhs, guess, diffusion):
    position = lax.axis_index("tm")
    cells = rhs.shape[1] * lax.axis_size("space") * rhs.shape[2]
    partials = []

    def weight_of(level):
        if level <= 1:
            return jnp.float32(1.0)
        stride = stride_of(level)
        return jnp.where(position % stride == stride - 1, 1.0, 0.0).astype(jnp.float32)

    def record(resid, level):
        local_part = jnp.sum(resid * resid) * weight_of(level)
        partials.append(local_part)

    sources = [rhs]
    fields = []
    field = guess
    for level in range(LEVELS - 1):
        source = sources[level]
        scaled = 2.0**level * diffusion
        diag = 1.0 + 4.0 * scaled
        stride = stride_of(level)
        if level == 0:
            field = field + damping * residual(field, source, scaled, diag, stride) / diag
        else:
            field = damping * source / diag
        resid = residual(field, source, scaled, diag, stride)
        record(resid, level)
        fields.append(field)
        if level == 0:
            coarse = resid[0:1] + resid[1:2]
        else:
            coarse = resid + from_partner(resid, "tm", level - 1)
        sources.append(coarse)
    level = LEVELS - 1
    source = sources[level]
    scaled = 2.0**level * diffusion
    diag = 1.0 + 4.0 * scaled
    stride = stride_of(level)
    field = damping * source / diag
    field = field + damping * residual(field, source, scaled, diag, stride) / diag
    resid = residual(field, source, scaled, diag, stride)
    record(resid, level)
    correction = field
    for level in range(LEVELS - 2, -1, -1):
        scaled = 2.0**level * diffusion
        diag = 1.0 + 4.0 * scaled
        stride = stride_of(level)
        field = fields[level] + correction
        field = field + damping * residual(field, sources[level], scaled, diag, stride) / diag
        correction = field
    scaled = 1.0 * diffusion
    diag = 1.0 + 4.0 * scaled
    resid = residual(correction, rhs, scaled, diag, 1)
    record(resid, 0)
    totals = lax.psum(jnp.stack(partials), ("tm", "space"))
    norms = jnp.sqrt(totals / cells)
    return (correction, norms)


DEVICE = pl.DeviceIdType.MESH
TILE = 8
EDGE = 2 * TILE
BLOCK = 32


def cycle_kernel(
    strips, devices, cells,
    rhs_in, guess_in, diff_in, out, norms_out,
    rhs, guess, diff, v0, g1, v1, r1, v1f, sol, guess_e, v0_e, v1_e, v1f_e, sol_e,
    pair, g2h, v2, c_g2, c_v2, c_g3, c_v3, c_g4, c_v4, c_v4b, finals, weights, tile, gathered, gathered_z,
    load_sem, store_sem, zs_sem, zr_sem, ts_sem, tr_sem, ps_sem, pr_sem, as_sem, ar_sem, al_sem,
    bs_sem, br_sem, bl_sem, rs_sem, credit, ns_sem, nr_sem, ms_sem, mr_sem,
):
    me = lax.axis_index("tm")
    strip = lax.axis_index("space")
    rows, width = rhs_in.shape[1], rhs_in.shape[2]
    chips = devices // 2
    core = lax.rem(me, 2)
    chip = me // 2
    low, high = EDGE, EDGE + rows
    first, last = me == 0, me == devices - 1
    top, bottom = strip == 0, strip == strips - 1
    piece = rows // devices

    def aligned(value):
        return pl.multiple_of(value, TILE)

    def tm_copy(src, dst, send, recv, target):
        return pltpu.make_async_remote_copy(
            src_ref=src, dst_ref=dst, send_sem=send, recv_sem=recv,
            device_id={"tm": target, "space": strip}, device_id_type=DEVICE,
        )

    def space_copy(src, dst, send, recv, target):
        return pltpu.make_async_remote_copy(
            src_ref=src, dst_ref=dst, send_sem=send, recv_sem=recv,
            device_id={"tm": me, "space": target}, device_id_type=DEVICE,
        )

    later = jnp.minimum(me + 1, devices - 1)
    loads = [
        pltpu.make_async_copy(guess_in, guess.at[:, low:high], load_sem.at[0]),
        pltpu.make_async_copy(diff_in, diff.at[low:high], load_sem.at[1]),
        pltpu.make_async_copy(rhs_in, rhs.at[:, low:high], load_sem.at[2]),
    ]
    for copy in loads:
        copy.start()

    barrier = pltpu.get_barrier_semaphore()
    for i in range(1, devices):
        pl.semaphore_signal(
            barrier, inc=1, device_id={"tm": lax.rem(me + i, devices), "space": strip}, device_id_type=DEVICE
        )
    for i in range(1, strips):
        pl.semaphore_signal(
            barrier, inc=1, device_id={"tm": me, "space": lax.rem(strip + i, strips)}, device_id_type=DEVICE
        )
    pl.semaphore_wait(barrier, devices + strips - 2)

    down = jnp.minimum(strip + 1, strips - 1)
    up = jnp.maximum(strip - 1, 0)

    def halo_pair(index, tail, head, low_dst, high_dst):
        return (
            space_copy(tail, low_dst, zs_sem.at[index, 0], zr_sem.at[index, 0], down),
            space_copy(head, high_dst, zs_sem.at[index, 1], zr_sem.at[index, 1], up),
        )

    before_low, after_high = slice(low - TILE, low), slice(high, high + TILE)
    halos = [
        halo_pair(
            0, guess_in.at[:, rows - TILE:rows], guess_in.at[:, 0:TILE],
            guess.at[:, before_low], guess.at[:, after_high],
        ),
        halo_pair(
            1, diff_in.at[rows - TILE:rows], diff_in.at[0:TILE], diff.at[before_low], diff.at[after_high],
        ),
        halo_pair(
            2, rhs_in.at[:, rows - TILE:rows], rhs_in.at[:, 0:TILE],
            rhs.at[:, before_low], rhs.at[:, after_high],
        ),
    ]

    def start_halo(pair_of):
        @pl.when(jnp.logical_not(bottom))
        def _():
            pair_of[0].start()

        @pl.when(jnp.logical_not(top))
        def _():
            pair_of[1].start()

    def finish_halo(pair_of):
        @pl.when(jnp.logical_not(top))
        def _():
            pair_of[0].wait_recv()
            pair_of[1].wait_send()

        @pl.when(jnp.logical_not(bottom))
        def _():
            pair_of[1].wait_recv()
            pair_of[0].wait_send()

    for pair_of in halos:
        start_halo(pair_of)

    half = rows // 2
    quarter = rows // 4
    whole = [
        (low - TILE, quarter + TILE), (low + quarter, quarter),
        (low + 2 * quarter, quarter), (low + 3 * quarter, quarter + TILE),
    ]
    inner = [(low + quarter * j, quarter) for j in range(4)]
    guess_parts = [(low, half), (low + half, half), (low - TILE, TILE), (high, TILE)]

    def shift(stage, source, target, parts):
        return [
            tm_copy(
                source(start, size), target.at[start:start + size],
                ts_sem.at[stage, j], tr_sem.at[stage, j], later,
            )
            for j, (start, size) in enumerate(parts)
        ]

    def send(copy):
        @pl.when(jnp.logical_not(last))
        def _():
            copy.start()

    def receive(copy):
        @pl.when(jnp.logical_not(first))
        def _():
            copy.wait_recv()

    guess_shift = shift(
        0,
        lambda start, size: (
            guess.at[1, start:start + size] if size == TILE else guess_in.at[1, start - low:start - low + size]
        ),
        guess_e, guess_parts,
    )
    v0_shift = shift(1, lambda start, size: v0.at[1, start:start + size], v0_e, whole)
    v1_shift = shift(2, lambda start, size: v1.at[start:start + size], v1_e, whole)
    v1f_shift = shift(3, lambda start, size: v1f.at[start:start + size], v1f_e, whole)
    sol_shift = shift(4, lambda start, size: sol.at[1, start:start + size], sol_e, inner)
    send(guess_shift[0])
    send(guess_shift[1])

    block = [TILE]

    def at(r):
        return pl.ds(r, block[0])

    def blocks(start, size, step, init=0, ahead=0):
        def loop(begin, count, tall, carry):
            def run(i, carry):
                return step(aligned(begin + i * tall), carry)

            block[0] = tall
            if count == 1:
                carry = step(aligned(begin), carry)
            elif count:
                carry = lax.fori_loop(0, count, run, carry)
            block[0] = TILE
            return carry

        carry = loop(start, ahead // TILE, TILE, init)
        count = (size - ahead) // BLOCK
        carry = loop(start + ahead, count, BLOCK, carry)
        done = ahead + count * BLOCK
        return loop(start + done, (size - done) // TILE, TILE, carry)

    @pl.when(first)
    def _():
        def clear(r, carry):
            zero = jnp.zeros((block[0], width), jnp.float32)
            for ref in (guess_e, v0_e, v1_e, v1f_e, sol_e):
                ref[at(r), :] = zero
            v2[1, at(r), :] = zero
            return carry

        blocks(low - TILE, rows + 2 * TILE, clear, 0, TILE)

    def chunk(j, step, init=0):
        start, size = whole[j]
        return blocks(start, size, step, init, TILE if j == 0 else 0)

    def clear_edge(start):
        for ref in (guess, rhs):
            for p in range(2):
                ref[p, start:start + TILE, :] = jnp.zeros((TILE, width), jnp.float32)
        for p in range(2):
            v2[p, start:start + TILE, :] = jnp.zeros((TILE, width), jnp.float32)
        diff[start:start + TILE, :] = jnp.zeros((TILE, width), jnp.float32)

    @pl.when(top)
    def _():
        clear_edge(low - TILE)

    @pl.when(bottom)
    def _():
        clear_edge(high)

    def stencil(tall):
        size = block[0]
        lane = lax.broadcasted_iota(jnp.int32, (size, width), 1)
        not_left, not_right = lane != 0, lane != width - 1
        mid = tall[TILE:TILE + size]
        total = tall[TILE - 1:TILE + size - 1] + tall[TILE + 1:TILE + size + 1]
        total = total + jnp.where(not_left, pltpu.roll(mid, 1, 1), 0.0)
        total = total + jnp.where(not_right, pltpu.roll(mid, width - 1, 1), 0.0)
        return mid, total

    def tall_at(r):
        return pl.ds(aligned(r - TILE), block[0] + 2 * TILE)

    def coefficients(level, r):
        scaled = 2.0**level * diff[at(r), :]
        diag = 1.0 + 4.0 * scaled
        if level < 2:
            return scaled, diag, weights[level, at(r), :]
        return scaled, diag, damping / diag

    def set_weights(r, carry):
        for level in range(2):
            weights[level, at(r), :] = damping / (1.0 + 4.0 * (2.0**level * diff[at(r), :]))
        return carry

    def squares(value, keep=None):
        square = value * value
        if keep is not None:
            square = jnp.where(keep, square, 0.0)
        total = square[:, 0:128]
        for i in range(1, width // 128):
            total = total + square[:, i * 128:(i + 1) * 128]
        folded = total[0:TILE]
        for i in range(TILE, block[0], TILE):
            folded = folded + total[i:i + TILE]
        return folded

    zero_tile = jnp.zeros((TILE, 128), jnp.float32)
    keep_share = 1.0 - damping

    def sweep_last(r, carry):
        scaled, _, weight = coefficients(0, r)
        mid, total = stencil(guess[1, tall_at(r), :])
        v0[1, at(r), :] = keep_share * mid + weight * (rhs[1, at(r), :] + scaled * total + guess[0, at(r), :])
        return carry

    for copy in loads:
        copy.wait()
    blocks(low, rows, set_weights)
    for j in (1, 2):
        chunk(j, sweep_last)
        send(v0_shift[j])
    finish_halo(halos[0])
    send(guess_shift[2])
    send(guess_shift[3])
    finish_halo(halos[1])
    finish_halo(halos[2])
    blocks(low - TILE, TILE, set_weights)
    blocks(high, TILE, set_weights)
    for j in (0, 3):
        chunk(j, sweep_last)
        send(v0_shift[j])

    def sweep_first(r, carry):
        scaled, _, weight = coefficients(0, r)
        mid, total = stencil(guess[0, tall_at(r), :])
        v0[0, at(r), :] = keep_share * mid + weight * (rhs[0, at(r), :] + scaled * total + guess_e[at(r), :])
        return carry

    for copy in guess_shift:
        receive(copy)
    for j in range(4):
        chunk(j, sweep_first)

    def descend(r, carry):
        keep = jnp.logical_and(r >= low, r < high)
        scaled, diag, _ = coefficients(0, r)
        mid, total = stencil(v0[0, tall_at(r), :])
        one = rhs[0, at(r), :] - diag * mid + scaled * total + v0_e[at(r), :]
        late, total = stencil(v0[1, tall_at(r), :])
        two = rhs[1, at(r), :] - diag * late + scaled * total + mid
        source = one + two
        g1[at(r), :] = source
        _, _, weight = coefficients(1, r)
        v1[at(r), :] = weight * source
        return carry + squares(one, keep) + squares(two, keep)

    total0 = zero_tile
    for j in range(4):
        receive(v0_shift[j])
        total0 = chunk(j, descend, total0)
        send(v1_shift[j])

    def residual1(r, carry):
        keep = jnp.logical_and(r >= low, r < high)
        scaled, _, _ = coefficients(1, r)
        _, total = stencil(v1[tall_at(r), :])
        resid = keep_share * g1[at(r), :] + scaled * total + v1_e[at(r), :]
        r1[at(r), :] = resid
        return carry + squares(resid, keep)

    total1 = zero_tile
    tall_piece = piece + 2 * TILE
    c_low, c_high = EDGE, EDGE + piece
    c_rows = slice(c_low - TILE, c_high + TILE)
    sibling = me + 1 - 2 * core

    def swap_of(k):
        start = low - TILE + k * piece
        return tm_copy(
            r1.at[start:start + tall_piece], pair.at[k // 2], ps_sem.at[k // 2], pr_sem.at[k // 2], sibling
        )

    def hand_over(k):
        return tm_copy(g2h.at[k // 2], c_g2.at[chip, c_rows], as_sem.at[k // 2], ar_sem.at[chip], k)

    def join_piece(k):
        start = low - TILE + k * piece

        def join(r, carry):
            g2h[k // 2, at(r), :] = r1[at(aligned(r + start)), :] + pair[k // 2, at(r), :]
            return carry

        swap_of(k).wait_recv()
        blocks(0, tall_piece, join, 0, TILE)
        local = pltpu.make_async_copy(g2h.at[k // 2], c_g2.at[chip, c_rows], al_sem)

        @pl.when(me == k)
        def _():
            local.start()
            local.wait()

        @pl.when(me != k)
        def _():
            hand_over(k).start()

    done = 0
    for j in range(4):
        receive(v1_shift[j])
        total1 = chunk(j, residual1, total1)
        ready = (sum(whole[j]) - tall_piece - low + TILE) // piece + 1
        for k in range(done, ready):
            @pl.when(core != k % 2)
            def _():
                swap_of(k).start()
        for k in range(done, ready):
            @pl.when(core == k % 2)
            def _():
                join_piece(k)
        done = ready
    for c in range(chips):
        copy = tm_copy(g2h.at[0], c_g2.at[c, c_rows], as_sem.at[0], ar_sem.at[c], sibling)

        @pl.when(c != chip)
        def _():
            copy.wait_recv()

    has_second = jnp.logical_and(core == 0, jnp.logical_not(first))

    offset = me * piece

    def coarse_coefficients(level, r):
        return coefficients(level, aligned(r + offset))


    def coarse(step, init=0):
        return blocks(c_low - TILE, tall_piece, step, init, TILE)

    def first_sweep(level, source, field, count):
        def step(r, carry):
            _, _, weight = coarse_coefficients(level, r)
            for p in range(count):
                field[p, at(r), :] = weight * source[p, at(r), :]
            return carry

        coarse(step)

    def coarse_residual(level, source, field, target, count):
        def step(r, carry):
            keep = jnp.logical_and(r >= c_low, r < c_high)
            scaled, _, _ = coarse_coefficients(level, r)
            earlier, even = None, None
            for p in range(count):
                mid, total = stencil(field[p, tall_at(r), :])
                resid = keep_share * source[p, at(r), :] + scaled * total
                if p:
                    resid = resid + earlier
                earlier = mid
                carry = carry + squares(resid, keep)
                if p % 2 == 0:
                    even = resid
                else:
                    target[p // 2, at(r), :] = even + resid
            return carry

        return coarse(step, zero_tile)

    def ascend(level, source, field, above, target, count):
        def step(r, carry):
            scaled, _, weight = coarse_coefficients(level, r)
            earlier = None
            for p in range(count):
                mid, total = stencil(field[p, tall_at(r), :] + above[p // 2, tall_at(r), :])
                value = source[p, at(r), :] + scaled * total
                if p:
                    value = value + earlier
                earlier = mid
                target[p, at(r), :] = keep_share * mid + weight * value
            return carry

        coarse(step)

    points2, points3 = chips, chips // 2
    first_sweep(2, c_g2, c_v2, points2)
    total2 = coarse_residual(2, c_g2, c_v2, c_g3, points2)
    first_sweep(3, c_g3, c_v3, points3)
    total3 = coarse_residual(3, c_g3, c_v3, c_g4, points3)
    first_sweep(4, c_g4, c_v4, 1)

    def second_sweep(r, carry):
        scaled, _, weight = coarse_coefficients(4, r)
        mid, total = stencil(c_v4[0, tall_at(r), :])
        c_v4b[0, at(r), :] = keep_share * mid + weight * (c_g4[0, at(r), :] + scaled * total)
        return carry

    coarse(second_sweep)

    def residual4(r, carry):
        scaled, diag, _ = coarse_coefficients(4, r)
        mid, total = stencil(c_v4b[0, tall_at(r), :])
        return carry + squares(c_g4[0, at(r), :] - diag * mid + scaled * total)

    total4 = blocks(c_low, piece, residual4, zero_tile)
    c_v3f, c_v2f = finals
    ascend(3, c_g3, c_v3, c_v4b, c_v3f, points3)
    ascend(2, c_g2, c_v2, c_v3f, c_v2f, points2)

    back = []
    place = pl.ds(aligned(low + offset), piece)
    for c in range(chips):
        wants = [(0, 2 * c + core, c)]
        if c > 0:
            wants.append((1, 2 * c, c - 1))
        for kind, target, point in wants:
            src, dst = c_v2f.at[point, c_low:c_high], v2.at[kind, place]
            copy = tm_copy(src, dst, bs_sem.at[kind, c], br_sem.at[kind, me], target)
            local = pltpu.make_async_copy(src, dst, bl_sem.at[kind])
            back.append((target, copy))

            @pl.when(me == target)
            def _():
                local.start()
                local.wait()

            @pl.when(me != target)
            def _():
                copy.start()

    relays = []
    for i in range(chips):
        for side in (core, 1 - core):
            k = 2 * i + side
            rows_of = pl.ds(aligned(low + k * piece), piece)
            arrival = tm_copy(v2.at[0, rows_of], v2.at[0, rows_of], rs_sem.at[i], br_sem.at[0, k], sibling)
            relays.append((k, arrival))
    for k, arrival in relays[0::2]:
        @pl.when(k != me)
        def _():
            arrival.wait_recv()

        arrival.start()
    for k, arrival in relays[1::2]:
        arrival.wait_recv()
    for k in range(devices):
        rows_of = slice(low + k * piece, low + (k + 1) * piece)
        arrival = tm_copy(v2.at[1, rows_of], v2.at[1, rows_of], bs_sem.at[1, 0], br_sem.at[1, k], sibling)

        @pl.when(jnp.logical_and(k != me, has_second))
        def _():
            arrival.wait_recv()

    v2_halos = [
        halo_pair(
            3 + kind, v2.at[kind, high - TILE:high], v2.at[kind, low:low + TILE],
            v2.at[kind, before_low], v2.at[kind, after_high],
        )
        for kind in range(2)
    ]
    start_halo(v2_halos[0])

    @pl.when(has_second)
    def _():
        start_halo(v2_halos[1])

    sends_on = jnp.logical_and(core == 1, jnp.logical_not(last))

    @pl.when(has_second)
    def _():
        pl.semaphore_signal(credit, inc=1, device_id={"tm": me - 1, "space": strip}, device_id_type=DEVICE)

    kind = 1 - core

    def ascend1(r, carry):
        scaled, _, weight = coefficients(1, r)
        mid, total = stencil(v1[tall_at(r), :] + v2[0, tall_at(r), :])
        earlier = v1_e[at(r), :] + v2[kind, at(r), :]
        v1f[at(r), :] = keep_share * mid + weight * (g1[at(r), :] + scaled * total + earlier)
        return carry

    for j in (1, 2, 0, 3):
        if j == 0:
            finish_halo(v2_halos[0])

            @pl.when(has_second)
            def _():
                finish_halo(v2_halos[1])

        chunk(j, ascend1)
        if j == 1:
            @pl.when(sends_on)
            def _():
                pl.semaphore_wait(credit, 1)
        send(v1f_shift[j])

    def ascend_last(r, carry):
        scaled, _, weight = coefficients(0, r)
        mid, total = stencil(v0[1, tall_at(r), :] + v1f[tall_at(r), :])
        earlier = v0[0, at(r), :] + v1f[at(r), :]
        sol[1, at(r), :] = keep_share * mid + weight * (rhs[1, at(r), :] + scaled * total + earlier)
        return carry

    blocks(low - TILE, TILE, ascend_last, 0)
    for start, size in inner:
        blocks(start, size, ascend_last, 0)
    blocks(high, TILE, ascend_last, 0)

    def ascend_first(r, carry):
        scaled, _, weight = coefficients(0, r)
        mid, total = stencil(v0[0, tall_at(r), :] + v1f[tall_at(r), :])
        earlier = v0_e[at(r), :] + v1f_e[at(r), :]
        sol[0, at(r), :] = keep_share * mid + weight * (rhs[0, at(r), :] + scaled * total + earlier)
        return carry

    for j in range(4):
        receive(v1f_shift[j])

        @pl.when(jnp.logical_not(last))
        def _():
            v1f_shift[j].wait_send()
            sol_shift[j].start()

        chunk(j, ascend_first)
    stores = pltpu.make_async_copy(sol.at[:, low:high], out, store_sem)
    stores.start()

    def final_last(r, carry):
        scaled, diag, _ = coefficients(0, r)
        mid, total = stencil(sol[1, tall_at(r), :])
        return carry + squares(rhs[1, at(r), :] - diag * mid + scaled * total + sol[0, at(r), :])

    total5 = blocks(low, rows, final_last, zero_tile)

    def final_first(r, carry):
        scaled, diag, _ = coefficients(0, r)
        mid, total = stencil(sol[0, tall_at(r), :])
        return carry + squares(rhs[0, at(r), :] - diag * mid + scaled * total + sol_e[at(r), :])

    for (start, size), arrived in zip(inner, sol_shift):
        receive(arrived)
        total5 = blocks(start, size, final_first, total5)

    parts = [total0, total1, total2, total3, total4, total5]
    for level, value in enumerate(parts):
        tile[level:level + 1, :] = jnp.sum(value, axis=0, keepdims=True)
    for level in range(len(parts), TILE):
        tile[level:level + 1, :] = jnp.zeros((1, 128), jnp.float32)

    def exchange(count, own, source, slots, copier, send_sems, recv_sems):
        slots[pl.ds(own, 1)] = source[...][None]
        sent = [
            copier(source, slots.at[own], send_sems.at[i], recv_sems.at[own], lax.rem(own + i, count))
            for i in range(1, count)
        ]
        for copy in sent:
            copy.start()
        for i in range(1, count):
            other = lax.rem(own + i, count)
            copier(source, slots.at[other], send_sems.at[i], recv_sems.at[other], other).wait_recv()
        for copy in sent:
            copy.wait_send()
        total = slots[0]
        for i in range(1, count):
            total = total + slots[i]
        return total

    total = exchange(devices, me, tile, gathered, tm_copy, ns_sem, nr_sem)
    tile[...] = total
    total = exchange(strips, strip, tile, gathered_z, space_copy, ms_sem, mr_sem)
    summed = jnp.sum(total, axis=1, keepdims=True)
    norms_out[...] = jnp.broadcast_to(jnp.sqrt(summed * (1.0 / cells)), (TILE, 128))

    stores.wait()
    for group in (guess_shift, v0_shift, v1_shift, sol_shift):
        for copy in group:
            @pl.when(jnp.logical_not(last))
            def _():
                copy.wait_send()
    for _, copy in relays[0::2]:
        copy.wait_send()
    for k in range(devices):
        @pl.when(core != k % 2)
        def _():
            swap_of(k).wait_send()

        @pl.when(jnp.logical_and(core == k % 2, me != k))
        def _():
            hand_over(k).wait_send()
    for target, copy in back:
        @pl.when(me != target)
        def _():
            copy.wait_send()


def fast_body(rhs, guess, diffusion):
    devices, strips = lax.axis_size("tm"), lax.axis_size("space")
    rows, width = rhs.shape[1:]
    chips = devices // 2
    cells = rows * strips * width
    height = rows + 2 * EDGE
    c_height = rows // devices + 2 * EDGE

    def plane(*lead):
        return pltpu.VMEM(lead + (height, width), jnp.float32)

    def coarse(count):
        return pltpu.VMEM((count, c_height, width), jnp.float32)

    shared = pltpu.VMEM((chips, rows // devices + EDGE, width), jnp.float32)
    dma = pltpu.SemaphoreType.DMA
    scratch = [
        plane(2), plane(2), plane(), plane(2), plane(), plane(), plane(), plane(), plane(2),
        plane(), plane(), plane(), plane(), plane(),
        shared, shared, plane(2),
        coarse(chips), coarse(chips), coarse(chips // 2), coarse(chips // 2), coarse(1), coarse(1), coarse(1),
        (coarse(chips // 2), coarse(chips)),
        plane(2),
        pltpu.VMEM((TILE, 128), jnp.float32),
        pltpu.VMEM((devices, TILE, 128), jnp.float32),
        pltpu.VMEM((strips, TILE, 128), jnp.float32),
        dma((3,)), dma, dma((5, 2)), dma((5, 2)), dma((5, 4)), dma((5, 4)), dma((chips,)), dma((chips,)),
        dma((chips,)), dma((chips,)), dma, dma((2, devices)), dma((2, devices)), dma((2,)),
        dma((chips,)), pltpu.SemaphoreType.REGULAR,
        dma((devices,)), dma((devices,)), dma((strips,)), dma((strips,)),
    ]
    any_space = pl.BlockSpec(memory_space=pl.ANY)
    result, norms = pl.pallas_call(
        functools.partial(cycle_kernel, strips, devices, cells),
        out_shape=(
            pltpu.VMEM(rhs.shape, jnp.float32),
            jax.ShapeDtypeStruct((TILE, 128), jnp.float32),
        ),
        in_specs=[any_space] * 3,
        out_specs=(pl.BlockSpec(memory_space=pltpu.VMEM), pl.BlockSpec(memory_space=pltpu.VMEM)),
        scratch_shapes=scratch,
        compiler_params=pltpu.CompilerParams(
            collective_id=0, has_side_effects=True, vmem_limit_bytes=67_043_328 - rhs.size * 4 - 2**17
        ),
    )(rhs, guess, diffusion)
    return result, norms[:LEVELS + 1, 0]


def solution(mesh):
    in_specs = (P("tm", "space", None), P("tm", "space", None), P("space", None))
    out_specs = (P("tm", "space", None), P())

    def choose(rhs, guess, diffusion):
        points = rhs.shape[0] * lax.axis_size("tm")
        one_coarsest = points == 2 ** (LEVELS - 1) and rhs.shape[0] == 2
        even = rhs.shape[1] % (TILE * lax.axis_size("tm")) == 0 and rhs.shape[2] % 128 == 0
        if one_coarsest and even:
            return fast_body(rhs, guess, diffusion)
        return body(rhs, guess, diffusion)

    return jax.shard_map(choose, mesh=mesh, in_specs=in_specs, out_specs=out_specs, check_vma=False)
```
